512 devices in a mesh: tm: 16 (over y, z_lo), slab: 32 (over x, z_hi, core).
Axes of the slice: x: 4, y: 8, z: 8 (z_hi: 4, z_lo: 2; z = z_hi * 2 + z_lo), core: 2. Of those that a mesh axis runs over, the one named last changes fastest.
Arguments:
- velocity: bfloat16 [16, 3, 2, 524288], P('tm', None, None, 'slab'), may hold values from -64 to 64
- shell_index: int32 [524288], P('slab'), may hold values from 0 to 127, as said below
- ref_order: int32 [16], replicated, may hold values from 0 to 15, each once
Outputs:
- coherence: float32 [16, 16, 128], P('tm')
- spectrum: float32 [16, 128], P('tm')
The draws below stay inside these ranges and needn't reach their ends.
Inputs may be any that keep to these rules, and one draw needn't show every extreme that they name: `shell_index`: every shell number from 0 to 127 is taken by some mode. `ref_order`: each snapshot number appears once.
All inputs are finite; a program needn't handle non-finite values.
Results may differ from the reference program's by a relative error of at most 0.0003.
Values may be sent and summed in bfloat16 or wider, within the bound.
A program may use at most 64 MiB of HBM per device.

```python
import math
import jax
import jax.numpy as jnp
from jax import lax

SHELLS = 128
SNAPS = 16
MODES = 524288


def draw_velocity(key, part):
    keys = jax.random.split(jax.random.fold_in(key, 11), 5)
    amplitude = jnp.exp(jax.random.uniform(keys[0], (MODES,), jnp.float32, 0.0, math.log(10.0)))
    noise = jnp.clip(jax.random.normal(keys[1], (SNAPS, 3, 2, MODES), jnp.float32), -4.0, 4.0)
    persist = jax.random.uniform(keys[2], (MODES,), jnp.float32, 0.3, 0.97)
    scaling = jnp.exp(jax.random.uniform(keys[3], (SNAPS, 64), jnp.float32, math.log(0.5), math.log(2.0)))
    turning = jax.random.uniform(keys[4], (MODES,), jnp.float32, 0.2, 1.0)
    keep_share = jnp.sqrt(1.0 - persist * persist)

    def advance(state, fresh):
        new_state = persist * state + keep_share * fresh
        return (new_state, new_state)
    last_state, states = lax.scan(advance, noise[0], noise[1:])
    states = jnp.concatenate([noise[0][None], states], axis=0)
    steps_taken = jnp.arange(SNAPS, dtype=jnp.int32).astype(jnp.float32)
    phase = steps_taken[:, None] * turning[None, :]
    cosine = jnp.cos(phase)[:, None, :]
    sine = jnp.sin(phase)[:, None, :]
    real_old = states[:, :, 0]
    imag_old = states[:, :, 1]
    real_new = real_old * cosine - imag_old * sine
    imag_new = real_old * sine + imag_old * cosine
    states = jnp.stack([real_new, imag_new], axis=2)
    position = jnp.arange(MODES, dtype=jnp.int32)
    band = position * 64 // MODES
    band_scale = scaling[:, band]
    values = states * amplitude[None, None, None, :] * band_scale[:, None, None, :]
    return jnp.clip(values, -64.0, 64.0).astype(jnp.bfloat16)


def draw_shell_index(key, part):
    first_draw = jax.random.randint(jax.random.fold_in(key, 23), (MODES,), 0, SHELLS, dtype=jnp.int32)
    second_draw = jax.random.randint(jax.random.fold_in(key, 29), (MODES,), 0, SHELLS, dtype=jnp.int32)
    drawn = jnp.maximum(first_draw, second_draw)
    position = jnp.arange(MODES, dtype=jnp.int32)
    stride = MODES // SHELLS
    forced = position // stride % SHELLS
    return jnp.where(position % stride == 0, forced, drawn).astype(jnp.int32)


def setup_inputs(seed: int = 0) -> dict:
    streams_of = jax.random.split(jax.random.key(seed), 4)
    velocity = draw_velocity(jax.random.fold_in(streams_of[3], 71), 0)
    shell_index = draw_shell_index(jax.random.fold_in(streams_of[3], 71), 0)
    ref_order = jax.random.permutation(streams_of[2], SNAPS).astype(jnp.int32)
    return dict(velocity=velocity, shell_index=shell_index, ref_order=ref_order)


def reference(velocity, shell_index, ref_order):
    fields = velocity.astype(jnp.float32)
    rotated = jnp.stack([fields[:, :, 1], -fields[:, :, 0]], axis=2)
    energy = jnp.sum(fields * fields, axis=(1, 2)).astype(jnp.bfloat16)
    energy = lax.optimization_barrier(energy).astype(jnp.float32)
    spectrum = jax.ops.segment_sum(energy.T, shell_index, num_segments=SHELLS).T

    def one_snapshot(snapshot):
        own_field = lax.dynamic_index_in_dim(fields, snapshot, 0, keepdims=False)
        own_rotated = lax.dynamic_index_in_dim(rotated, snapshot, 0, keepdims=False)
        real_part = jnp.einsum("cpm,scpm->sm", own_field, fields, precision=lax.Precision.HIGHEST)
        imag_part = jnp.einsum("cpm,scpm->sm", own_rotated, fields, precision=lax.Precision.HIGHEST)
        stacked = jnp.stack([real_part, imag_part], axis=0).astype(jnp.bfloat16)
        stacked = lax.optimization_barrier(stacked).astype(jnp.float32)
        binned = jax.ops.segment_sum(stacked.reshape(2 * SNAPS, MODES).T, shell_index, num_segments=SHELLS)
        return binned.T.reshape(2, SNAPS, SHELLS)

    pair_sums = lax.map(one_snapshot, jnp.arange(SNAPS, dtype=jnp.int32))
    chosen = pair_sums[:, :, ref_order]
    power_sum = chosen[:, 0] * chosen[:, 0] + chosen[:, 1] * chosen[:, 1]
    coherence = power_sum / (spectrum[:, None, :] * spectrum[ref_order][None, :, :])
    return coherence, spectrum
```

```python
import functools

import jax
import jax.numpy as jnp
from jax import lax
from jax.experimental import pallas as pl
from jax.experimental.pallas import tpu as pltpu
from jax.sharding import PartitionSpec as P

SHELLS = 128
LANES = 128
Z_LO, Z_HI, CORES = 2, 4, 2
MESH = pl.DeviceIdType.MESH
ROWS = 16
GROUPS = ROWS // 2
PITCH = ROWS + 1


def remote(src, dst, send_sem, recv_sem, tm, slab):
    return pltpu.make_async_remote_copy(
        src_ref=src,
        dst_ref=dst,
        send_sem=send_sem,
        recv_sem=recv_sem,
        device_id={"tm": tm, "slab": slab},
        device_id_type=MESH,
    )


def kernel(
    sizes,
    vel_ref,
    shell_ref,
    order_ref,
    coh_ref,
    spec_ref,
    src,
    recv,
    ids,
    wide,
    terms,
    onehot,
    sums,
    peer_sums,
    y_recv,
    x_recv,
    z_src,
    z_recv,
    own_msg,
    c_recv,
    coh_rows,
    load_sem,
    m_send,
    m_recv,
    d_send,
    d_recv,
    y_send,
    y_rsem,
    x_send,
    x_rsem,
    z_send,
    z_rsem,
    c_send,
    c_rsem,
    o_send,
    o_rsem,
):
    y_n, x_n, z_hi_n, z_lo_n = sizes
    snaps = y_n * z_lo_n
    half = snaps // 2
    z_n = z_hi_n * z_lo_n
    block = z_lo_n * snaps
    me = lax.axis_index("tm")
    slab = lax.axis_index("slab")
    y, z_lo = me // z_lo_n, me % z_lo_n
    core = slab % CORES
    chip_slab = slab // CORES
    x, z_hi = chip_slab // z_hi_n, chip_slab % z_hi_n
    z = z_hi * z_lo_n + z_lo
    far = slab - core
    near = far + 1

    def slab_of(xx, zz, cc):
        return (xx * z_hi_n + zz) * CORES + cc

    load_all = pltpu.make_async_copy(vel_ref, src, load_sem.at[0])
    load_all.start()
    mine = pl.ds(pl.multiple_of(me * ROWS, ROWS), ROWS)
    load_own = pltpu.make_async_copy(vel_ref.at[:, mine], recv.at[me], load_sem.at[1])
    load_own.start()
    load_ids = pltpu.make_async_copy(
        shell_ref.at[pl.ds(pl.multiple_of(me * GROUPS, GROUPS), GROUPS)], ids, load_sem.at[2]
    )
    load_ids.start()

    barrier = pltpu.get_barrier_semaphore()

    def greet(tm, sl):
        pl.semaphore_signal(barrier, inc=1, device_id={"tm": tm, "slab": sl}, device_id_type=MESH)

    for d in range(1, snaps):
        greet((me + d) % snaps, slab)

    @pl.when(core == 0)
    def _():
        greet(me, near)
        for d in range(1, snaps):
            greet((me + d) % snaps, near)
        pl.semaphore_wait(barrier, snaps)

    z_partners = [(zl, dz) for zl in range(z_lo_n) for dz in range(z_hi_n) if (zl, dz) != (0, 0)]

    @pl.when(core == 1)
    def _():
        greet(me, far)
        for d in range(1, x_n):
            greet(me, slab_of((x + d) % x_n, z_hi, 1))
        for zl, dz in z_partners:
            if dz:
                greet(y * z_lo_n + (z_lo + zl) % z_lo_n, slab_of(x, (z_hi + dz) % z_hi_n, 1))
        others = sum(1 for _, dz in z_partners if dz)
        pl.semaphore_wait(barrier, 2 * snaps - 1 + x_n - 1 + others)

    load_all.wait()
    m_copies = []
    for d in range(1, snaps):
        to = (me + d) % snaps
        part = pl.ds(pl.multiple_of(to * ROWS, ROWS), ROWS)
        copy = remote(src.at[:, part], recv.at[me], m_send.at[d], m_recv.at[d], to, slab)
        copy.start()
        m_copies.append(copy)

    load_ids.wait()
    shells = lax.broadcasted_iota(jnp.int32, (SHELLS, LANES), 0)
    for g in range(GROUPS):
        row = jnp.broadcast_to(ids[g : g + 1, :], (SHELLS, LANES))
        onehot[:, g * LANES : (g + 1) * LANES] = jnp.where(row == shells, 1.0, 0.0).astype(
            jnp.bfloat16
        )

    load_own.wait()
    for d in range(1, snaps):
        frm = (me + snaps - d) % snaps
        remote(
            src.at[:, pl.ds(0, ROWS)], recv.at[frm], m_send.at[d], m_recv.at[d], me, slab
        ).wait_recv()
    for t in range(snaps):
        for c in range(3):
            value = recv[t, c].astype(jnp.float32)
            wide[c, t * PITCH : t * PITCH + ROWS, :] = value
            if t < half:
                at = (t + snaps) * PITCH
                wide[c, at : at + ROWS, :] = value

    first = lax.broadcasted_iota(jnp.int32, (snaps, LANES), 0) < half
    for g in range(GROUPS):

        def rows(c, p, d):
            return wide[c, pl.ds(d * PITCH + 2 * g + p, snaps, stride=PITCH), :]

        own = [[rows(c, p, 0) for p in range(2)] for c in range(3)]

        def put(k, value):
            terms[k * snaps : (k + 1) * snaps, g * LANES : (g + 1) * LANES] = value.astype(
                jnp.bfloat16
            )

        put(0, sum(own[c][p] * own[c][p] for c in range(3) for p in range(2)))
        for d in range(1, half + 1):
            other = [[rows(c, p, d) for p in range(2)] for c in range(3)]
            real = sum(own[c][p] * other[c][p] for c in range(3) for p in range(2))
            imag = sum(own[c][1] * other[c][0] - own[c][0] * other[c][1] for c in range(3))
            if d < half:
                put(2 * d - 1, real)
                put(2 * d, imag)
            else:
                put(2 * d - 1, jnp.where(first, real, imag))

    binned = lax.dot_general(
        terms[...], onehot[...], (((1,), (1,)), ((), ())), preferred_element_type=jnp.float32
    )
    for k in range(snaps):
        sums[pl.ds(k, snaps, stride=snaps), :] = binned[k * snaps : (k + 1) * snaps]

    def to_near():
        return remote(sums, peer_sums, d_send, d_recv, me, near)

    @pl.when(core == 0)
    def _():
        to_near().start()

    @pl.when(core == 1)
    def _():
        to_near().wait_recv()
        sums[...] += peer_sums[...]

        def y_block(yy):
            return pl.ds(pl.multiple_of(yy * block, block), block)

        for d in range(1, y_n):
            yy = (y + d) % y_n
            remote(
                sums.at[y_block(yy)],
                y_recv.at[y],
                y_send.at[d],
                y_rsem.at[d],
                yy * z_lo_n + z_lo,
                slab,
            ).start()
        y_recv[y] = sums[y_block(y), :]
        for d in range(1, y_n):
            frm = (y + y_n - d) % y_n
            remote(
                sums.at[y_block(0)], y_recv.at[frm], y_send.at[d], y_rsem.at[d], me, slab
            ).wait_recv()
        x_recv[x] = sum((y_recv[i] for i in range(1, y_n)), y_recv[0])

        for d in range(1, x_n):
            xx = (x + d) % x_n
            remote(
                x_recv.at[x], x_recv.at[x], x_send.at[d], x_rsem.at[d], me, slab_of(xx, z_hi, 1)
            ).start()
        for d in range(1, x_n):
            frm = (x + x_n - d) % x_n
            remote(
                x_recv.at[x], x_recv.at[frm], x_send.at[d], x_rsem.at[d], me, slab
            ).wait_recv()
        over_x = sum((x_recv[i] for i in range(1, x_n)), x_recv[0])
        for i in range(z_lo_n):
            z_src[i] = over_x[i * snaps : (i + 1) * snaps]

        for n, (zl, dz) in enumerate(z_partners):
            to_lo, to_hi = (z_lo + zl) % z_lo_n, (z_hi + dz) % z_hi_n
            remote(
                z_src.at[to_lo],
                z_recv.at[z],
                z_send.at[n],
                z_rsem.at[n],
                y * z_lo_n + to_lo,
                slab_of(x, to_hi, 1),
            ).start()
        z_recv[z] = z_src[z_lo]
        for n, (zl, dz) in enumerate(z_partners):
            from_lo, from_hi = (z_lo + z_lo_n - zl) % z_lo_n, (z_hi + z_hi_n - dz) % z_hi_n
            frm = from_hi * z_lo_n + from_lo
            remote(
                z_src.at[0], z_recv.at[frm], z_send.at[n], z_rsem.at[n], me, slab
            ).wait_recv()
        total = sum((z_recv[i] for i in range(1, z_n)), z_recv[0])

        own_spec = total[0:1]
        for d in range(snaps):
            own_msg[d, 0:1, :] = own_spec
            if 0 < d < half:
                re, im = total[2 * d - 1 : 2 * d], total[2 * d : 2 * d + 1]
                own_msg[d, 1:2, :] = re * re + im * im
            elif d == half:
                row = total[2 * d - 1 : 2 * d]
                own_msg[d, 1:2, :] = row * row
            else:
                own_msg[d, 1:2, :] = own_spec * own_spec
        for d in range(1, snaps):
            to = (me + d) % snaps
            for cc in range(CORES):
                remote(
                    own_msg.at[d], c_recv.at[d], c_send.at[cc, d], c_rsem.at[d], to, far + cc
                ).start()
        remote(own_msg, own_msg, o_send, o_rsem, me, far).start()

    @pl.when(core == 0)
    def _():
        remote(own_msg, own_msg, o_send, o_rsem, me, near).wait_recv()

    for d in range(1, snaps):
        remote(own_msg.at[d], c_recv.at[d], c_send.at[0, d], c_rsem.at[d], me, slab).wait_recv()

    spec = own_msg[0, 0:1, :]
    spec_ref[...] = spec
    coh_rows[0] = own_msg[0, 1:2, :] / (spec * spec)
    for e in range(1, snaps):
        if e < half:
            power = c_recv[e, 1:2, :]
        elif e == half:
            power = c_recv[e, 1:2, :] + own_msg[e, 1:2, :]
        else:
            power = own_msg[snaps - e, 1:2, :]
        coh_rows[e] = power / (spec * c_recv[e, 0:1, :])
    for j in range(snaps):
        coh_ref[0, j : j + 1, :] = coh_rows[(me - order_ref[j] + snaps) % snaps]

    for copy in m_copies:
        copy.wait_send()

    @pl.when(core == 0)
    def _():
        to_near().wait_send()

    @pl.when(core == 1)
    def _():
        for d in range(1, y_n):
            remote(
                sums.at[pl.ds(0, block)], y_recv.at[0], y_send.at[d], y_rsem.at[d], me, slab
            ).wait_send()
        for d in range(1, x_n):
            remote(x_recv.at[x], x_recv.at[x], x_send.at[d], x_rsem.at[d], me, slab).wait_send()
        for n in range(len(z_partners)):
            remote(z_src.at[0], z_recv.at[0], z_send.at[n], z_rsem.at[n], me, slab).wait_send()
        for d in range(1, snaps):
            for cc in range(CORES):
                remote(
                    own_msg.at[d], c_recv.at[d], c_send.at[cc, d], c_rsem.at[d], me, slab
                ).wait_send()
        remote(own_msg, own_msg, o_send, o_rsem, me, far).wait_send()


def body(sizes, velocity, shell_index, ref_order):
    y_n, x_n, z_hi_n, z_lo_n = sizes
    snaps = y_n * z_lo_n
    half = snaps // 2
    z_n = z_hi_n * z_lo_n
    lanes_n = velocity.shape[3] // LANES
    vel = velocity.reshape(3, 2, lanes_n, LANES).transpose(0, 2, 1, 3)
    vel = vel.reshape(3, 2 * lanes_n, LANES)
    ids = shell_index.reshape(lanes_n, LANES)
    f32, dma = jnp.float32, pltpu.SemaphoreType.DMA
    return pl.pallas_call(
        functools.partial(kernel, sizes),
        out_shape=(
            jax.ShapeDtypeStruct((1, snaps, SHELLS), f32),
            jax.ShapeDtypeStruct((1, SHELLS), f32),
        ),
        in_specs=[
            pl.BlockSpec(memory_space=pl.ANY),
            pl.BlockSpec(memory_space=pl.ANY),
            pl.BlockSpec(memory_space=pltpu.SMEM),
        ],
        out_specs=(pl.BlockSpec(memory_space=pltpu.VMEM), pl.BlockSpec(memory_space=pltpu.VMEM)),
        scratch_shapes=[
            pltpu.VMEM((3, 2 * lanes_n, LANES), jnp.bfloat16),
            pltpu.VMEM((snaps, 3, ROWS, LANES), jnp.bfloat16),
            pltpu.VMEM((GROUPS, LANES), jnp.int32),
            pltpu.VMEM((3, (snaps + half + 1) * PITCH, LANES), f32),
            pltpu.VMEM((snaps * snaps, GROUPS * LANES), jnp.bfloat16),
            pltpu.VMEM((SHELLS, GROUPS * LANES), jnp.bfloat16),
            pltpu.VMEM((snaps * snaps, SHELLS), f32),
            pltpu.VMEM((snaps * snaps, SHELLS), f32),
            pltpu.VMEM((y_n, z_lo_n * snaps, SHELLS), f32),
            pltpu.VMEM((x_n, z_lo_n * snaps, SHELLS), f32),
            pltpu.VMEM((z_lo_n, snaps, SHELLS), f32),
            pltpu.VMEM((z_n, snaps, SHELLS), f32),
            pltpu.VMEM((snaps, 2, SHELLS), f32),
            pltpu.VMEM((snaps, 2, SHELLS), f32),
            pltpu.VMEM((snaps, 1, SHELLS), f32),
            dma((3,)),
            dma((snaps,)),
            dma((snaps,)),
            dma(()),
            dma(()),
            dma((y_n,)),
            dma((y_n,)),
            dma((x_n,)),
            dma((x_n,)),
            dma((z_n,)),
            dma((z_n,)),
            dma((CORES, snaps)),
            dma((snaps,)),
            dma(()),
            dma(()),
        ],
        compiler_params=pltpu.CompilerParams(collective_id=0, has_side_effects=True),
    )(vel, ids, ref_order)


def solution(mesh):
    tm, slab = mesh.shape["tm"], mesh.shape["slab"]
    z_hi_n = min(Z_HI, slab // CORES)
    sizes = (tm // Z_LO, slab // CORES // z_hi_n, z_hi_n, Z_LO)
    return jax.shard_map(
        functools.partial(body, sizes),
        mesh=mesh,
        in_specs=(P("tm", None, None, "slab"), P("slab"), P()),
        out_specs=(P("tm", None, None), P("tm", None)),
        check_vma=False,
    )
```

```python
import functools

import jax
import jax.numpy as jnp
from jax import lax
from jax.experimental import pallas as pl
from jax.experimental.pallas import tpu as pltpu
from jax.sharding import PartitionSpec as P

SHELLS = 128
LANES = 128
Z_LO, Z_HI, CORES = 2, 4, 2
ROWS = 16
GROUPS = ROWS // 2
PITCH = ROWS + 1
OUT_ROWS = 24


def remote(src, dst, send_sem, recv_sem, tm, slab):
    return pltpu.make_async_remote_copy(
        src_ref=src,
        dst_ref=dst,
        send_sem=send_sem,
        recv_sem=recv_sem,
        device_id={"tm": tm, "slab": slab},
        device_id_type=pl.DeviceIdType.MESH,
    )


def ordered_sum(terms):
    total = terms[0]
    for term in terms[1:]:
        total = total + term
    return total


def kernel(
    sizes,
    vel_ref,
    shell_ref,
    order_hbm,
    out_ref,
    src,
    recv,
    ids,
    order_ref,
    wide,
    terms,
    onehot,
    sums,
    r_recv,
    x_recv,
    own_src,
    own_recv,
    pair_src,
    pair_recv,
    coh_rows,
    final,
    load_sem,
    m_send,
    m_recv,
    i_send,
    i_recv,
    r_send,
    r_rsem,
    x_send,
    x_rsem,
    p_send,
    p_rsem,
    f_send,
    f_rsem,
):
    snaps, x_n, z_hi_n = sizes
    half = snaps // 2
    heads = min(2, z_hi_n)
    me = lax.axis_index("tm")
    slab = lax.axis_index("slab")
    core = slab % CORES
    x, z_hi = slab // CORES // z_hi_n, slab // CORES % z_hi_n
    far = slab - core
    near = far + 1
    by_distance = sorted(range(1, snaps), key=lambda d: (-min(d, snaps - d), d))

    def there(d):
        return (me + d) % snaps

    def whence(d):
        return (me + snaps - d) % snaps

    def slab_of(xx, zz, cc):
        return (xx * z_hi_n + zz) * CORES + cc

    def rows_of(t, n):
        return pl.ds(pl.multiple_of(t * n, n), n)

    load_all = pltpu.make_async_copy(vel_ref, src, load_sem.at[0])
    load_all.start()
    load_ids = pltpu.make_async_copy(
        shell_ref.at[rows_of(me, GROUPS)], ids.at[core], load_sem.at[1]
    )
    load_own = pltpu.make_async_copy(
        vel_ref.at[:, rows_of(me, ROWS)], recv.at[1, me], load_sem.at[2]
    )
    load_order = pltpu.make_async_copy(order_hbm, order_ref, load_sem.at[3])

    barrier = pltpu.get_barrier_semaphore()

    def greet(tm, sl):
        pl.semaphore_signal(
            barrier, inc=1, device_id={"tm": tm, "slab": sl}, device_id_type=pl.DeviceIdType.MESH
        )

    with jax.named_scope("a_greet"):

        @pl.when(core == 1)
        def _():
            for d in by_distance:
                greet(there(d), near)
                greet(there(d), far)
            greet(me, far)
            for d in range(1, x_n):
                greet(there(0), slab_of((x + d) % x_n, z_hi, 1))

        load_ids.start()

        @pl.when(core == 1)
        def _():
            load_own.start()
            load_order.start()

            @pl.when(z_hi < heads)
            def _():
                for h in range(1, z_hi_n):
                    for d in range(snaps):
                        greet(there(d), slab_of(x, (z_hi + h) % z_hi_n, 1))

    with jax.named_scope("b_barrier"):

        @pl.when(core == 0)
        def _():
            pl.semaphore_wait(barrier, snaps)

        @pl.when(core == 1)
        def _():
            @pl.when(z_hi < heads)
            def _():
                pl.semaphore_wait(barrier, snaps - 1 + x_n - 1 + (heads - 1) * snaps)

            @pl.when(z_hi >= heads)
            def _():
                pl.semaphore_wait(barrier, snaps - 1 + x_n - 1 + heads * snaps)

    def part_copy(d):
        return remote(
            src.at[:, rows_of(there(d), ROWS)],
            recv.at[core, me],
            m_send.at[d],
            m_recv.at[core, d],
            there(d),
            near,
        )

    def ids_copy():
        return remote(ids.at[0], ids.at[0], i_send, i_recv, me, near)

    load_all.wait()
    for d in by_distance:
        part_copy(d).start()

    @pl.when(core == 0)
    def _():
        part_copy(0).start()
        load_ids.wait()
        ids_copy().start()

    @pl.when(core == 1)
    def _():
        shells = lax.broadcasted_iota(jnp.int32, (SHELLS, LANES), 0)
        first = lax.broadcasted_iota(jnp.int32, (snaps, LANES), 0) < half

        def spread_shells(c):
            for g in range(GROUPS):
                row = jnp.broadcast_to(ids[c, g : g + 1, :], (SHELLS, LANES))
                hot = jnp.where(row == shells, 1.0, 0.0).astype(jnp.bfloat16)
                onehot[c, :, g * LANES : (g + 1) * LANES] = hot

        def widen(core_of):
            for t in range(snaps):
                for c in range(3):
                    value = recv[core_of, t, c].astype(jnp.float32)
                    wide[c, t * PITCH : t * PITCH + ROWS, :] = value
                    if t < half:
                        at = (t + snaps) * PITCH
                        wide[c, at : at + ROWS, :] = value

        def products():
            for g in range(GROUPS):

                def rows(c, p, d):
                    return wide[c, pl.ds(d * PITCH + 2 * g + p, snaps, stride=PITCH), :]

                def put(k, value):
                    terms[k * snaps : (k + 1) * snaps, g * LANES : (g + 1) * LANES] = value.astype(
                        jnp.bfloat16
                    )

                own = [[rows(c, p, 0) for p in range(2)] for c in range(3)]
                put(0, sum(own[c][p] * own[c][p] for c in range(3) for p in range(2)))
                for d in range(1, half + 1):
                    other = [[rows(c, p, d) for p in range(2)] for c in range(3)]
                    real = sum(own[c][p] * other[c][p] for c in range(3) for p in range(2))
                    imag = sum(own[c][1] * other[c][0] - own[c][0] * other[c][1] for c in range(3))
                    if d < half:
                        put(2 * d - 1, real)
                        put(2 * d, imag)
                    else:
                        put(2 * d - 1, jnp.where(first, real, imag))

        def binned(c):
            return lax.dot_general(
                terms[...],
                onehot[c],
                (((1,), (1,)), ((), ())),
                preferred_element_type=jnp.float32,
            )

        def wait_part(c, d):
            remote(
                src.at[:, pl.ds(0, ROWS)],
                recv.at[c, whence(d)],
                m_send.at[d],
                m_recv.at[c, d],
                me,
                slab,
            ).wait_recv()

        with jax.named_scope("c_onehot"):
            load_ids.wait()
            spread_shells(1)
            ids_copy().wait_recv()
            spread_shells(0)
        with jax.named_scope("d_wait1"):
            load_own.wait()
            for d in reversed(by_distance):
                wait_part(1, d)
        with jax.named_scope("e_work1"):
            widen(1)
            products()
            sums[...] = binned(1)
        with jax.named_scope("f_wait0"):
            for d in [0, *reversed(by_distance)]:
                wait_part(0, d)
        with jax.named_scope("g_work0"):
            widen(0)
            products()
            both = sums[...] + binned(0)
            for k in range(snaps):
                sums[pl.ds(k, snaps, stride=snaps), :] = both[k * snaps : (k + 1) * snaps]

        with jax.named_scope("h_owner"):
            for d in by_distance:
                remote(
                    sums.at[rows_of(there(d), snaps)],
                    r_recv.at[me],
                    r_send.at[d],
                    r_rsem.at[d],
                    there(d),
                    slab,
                ).start()
            r_recv[me] = sums[rows_of(me, snaps), :]
            for d in reversed(by_distance):
                remote(
                    sums.at[pl.ds(0, snaps)],
                    r_recv.at[whence(d)],
                    r_send.at[d],
                    r_rsem.at[d],
                    me,
                    slab,
                ).wait_recv()
            x_recv[x] = ordered_sum([r_recv[t] for t in range(snaps)])

        with jax.named_scope("i_x"):
            for d in range(1, x_n):
                remote(
                    x_recv.at[x],
                    x_recv.at[x],
                    x_send.at[d],
                    x_rsem.at[d],
                    me,
                    slab_of((x + d) % x_n, z_hi, 1),
                ).start()
            for d in range(1, x_n):
                remote(
                    x_recv.at[x],
                    x_recv.at[(x + x_n - d) % x_n],
                    x_send.at[d],
                    x_rsem.at[d],
                    me,
                    slab,
                ).wait_recv()
            total = ordered_sum([x_recv[i] for i in range(x_n)])

        with jax.named_scope("j_pairs"):
            own_src[...] = total
            for d in range(1, snaps):
                pair_src[d, 0, 0:1, :] = total[0:1]
                if d < half:
                    pair_src[d, 1, :, :] = total[2 * d - 1 : 2 * d + 1]
                elif d == half:
                    pair_src[d, 1, 0:1, :] = total[2 * d - 1 : 2 * d]
                    pair_src[d, 1, 1:2, :] = jnp.zeros((1, SHELLS), jnp.float32)
                pair_src[d, 0, 1:2, :] = jnp.zeros((1, SHELLS), jnp.float32)

        def pair_ref(ref, d):
            return ref.at[d] if d <= half else ref.at[d, 0]

        def pair_send(h, d):
            return remote(
                pair_ref(pair_src, d),
                pair_ref(pair_recv.at[z_hi], d),
                p_send.at[h, d],
                p_rsem.at[z_hi, d],
                there(d),
                slab_of(x, h, 1),
            )

        def own_send(h):
            return remote(
                own_src,
                own_recv.at[z_hi],
                p_send.at[h, 0],
                p_rsem.at[z_hi, 0],
                me,
                slab_of(x, h, 1),
            )

        with jax.named_scope("k_send"):
            for h in range(heads):
                for d in by_distance:
                    pair_send(h, d).start()

                @pl.when(z_hi != h)
                def _(h=h):
                    own_send(h).start()

                @pl.when(z_hi == h)
                def _(h=h):
                    own_recv[h] = own_src[...]

        def to_late(c):
            return remote(
                final,
                final,
                f_send.at[c],
                f_rsem,
                me,
                slab_of(x, z_hi_n - 1 - z_hi, c),
            )

        def to_partner():
            return remote(final, final, f_send.at[2], f_rsem, me, far)

        @pl.when(z_hi < heads)
        def _():
            with jax.named_scope("l_pairwait"):
                for h in range(z_hi_n):
                    for d in reversed(by_distance):
                        remote(
                            pair_ref(pair_src, d),
                            pair_ref(pair_recv.at[h], d),
                            p_send.at[0, d],
                            p_rsem.at[h, d],
                            me,
                            slab,
                        ).wait_recv()

                    @pl.when(z_hi != h)
                    def _(h=h):
                        remote(
                            own_src, own_recv.at[h], p_send.at[0, 0], p_rsem.at[h, 0], me, slab
                        ).wait_recv()

            with jax.named_scope("m_coh"):
                load_order.wait()
                own = ordered_sum([own_recv[h] for h in range(z_hi_n)])
                spec = own[0:1]
                energy = [spec] + [
                    ordered_sum([pair_recv[h, d, 0, 0:1, :] for h in range(z_hi_n)])
                    for d in range(1, snaps)
                ]
                final[snaps : snaps + 1, :] = spec
                coh_rows[0] = spec * spec / (spec * spec)
                for e in range(1, snaps):
                    if e <= half:
                        pair = ordered_sum([pair_recv[h, e, 1] for h in range(z_hi_n)])
                        re, im = pair[0:1], pair[1:2]
                        if e == half:
                            im = own[2 * e - 1 : 2 * e]
                    else:
                        d = snaps - e
                        re, im = own[2 * d - 1 : 2 * d], own[2 * d : 2 * d + 1]
                    coh_rows[e] = (re * re + im * im) / (spec * energy[e])
                for j in range(snaps):
                    final[j : j + 1, :] = coh_rows[(me - order_ref[j] + snaps) % snaps]
                to_partner().start()

                @pl.when(z_hi_n - 1 - z_hi >= heads)
                def _():
                    for c in (1, 0):
                        to_late(c).start()

        @pl.when(z_hi >= heads)
        def _():
            with jax.named_scope("n_finalwait"):
                remote(final, final, f_send.at[0], f_rsem, me, slab).wait_recv()
                load_order.wait()

    @pl.when(core == 0)
    def _():
        with jax.named_scope("n_finalwait"):
            remote(final, final, f_send.at[0], f_rsem, me, slab).wait_recv()

    with jax.named_scope("o_end"):
        out_ref[...] = final[0 : snaps + 1]
        for d in by_distance:
            part_copy(d).wait_send()

        @pl.when(core == 0)
        def _():
            part_copy(0).wait_send()
            ids_copy().wait_send()

        @pl.when(core == 1)
        def _():
            for d in range(1, snaps):
                remote(
                    sums.at[pl.ds(0, snaps)], r_recv.at[0], r_send.at[d], r_rsem.at[d], me, slab
                ).wait_send()
            for d in range(1, x_n):
                remote(
                    x_recv.at[x], x_recv.at[x], x_send.at[d], x_rsem.at[d], me, slab
                ).wait_send()
            for h in range(heads):
                for d in range(1, snaps):
                    ref = pair_src.at[d] if d <= half else pair_src.at[d, 0]
                    remote(ref, ref, p_send.at[h, d], p_rsem.at[0, d], me, slab).wait_send()

                @pl.when(z_hi != h)
                def _(h=h):
                    remote(
                        own_src, own_src, p_send.at[h, 0], p_rsem.at[0, 0], me, slab
                    ).wait_send()

            @pl.when(z_hi < heads)
            def _():
                remote(final, final, f_send.at[2], f_rsem, me, slab).wait_send()

                @pl.when(z_hi_n - 1 - z_hi >= heads)
                def _():
                    for c in (1, 0):
                        remote(final, final, f_send.at[c], f_rsem, me, slab).wait_send()


def finish(snaps, done_ref, coh_ref, spec_ref, sem):
    coh = pltpu.make_async_copy(done_ref.at[0:snaps], coh_ref.at[0], sem.at[0])
    spec = pltpu.make_async_copy(done_ref.at[snaps : snaps + 1], spec_ref, sem.at[1])
    coh.start()
    spec.start()
    coh.wait()
    spec.wait()


def body(sizes, velocity, shell_index, ref_order):
    snaps, x_n, z_hi_n = sizes
    half = snaps // 2
    heads = min(2, z_hi_n)
    lanes_n = velocity.shape[3] // LANES
    vel = velocity.reshape(3, 2, lanes_n, LANES).transpose(0, 2, 1, 3)
    vel = vel.reshape(3, 2 * lanes_n, LANES)
    ids = shell_index.reshape(lanes_n, LANES)
    f32, bf16, dma = jnp.float32, jnp.bfloat16, pltpu.SemaphoreType.DMA
    done = pl.pallas_call(
        functools.partial(kernel, sizes),
        out_shape=pltpu.VMEM((snaps + 1, SHELLS), f32),
        in_specs=[pl.BlockSpec(memory_space=pl.ANY)] * 3,
        out_specs=pl.BlockSpec(memory_space=pltpu.VMEM),
        scratch_shapes=[
            pltpu.VMEM((3, 2 * lanes_n, LANES), bf16),
            pltpu.VMEM((CORES, snaps, 3, ROWS, LANES), bf16),
            pltpu.VMEM((CORES, GROUPS, LANES), jnp.int32),
            pltpu.SMEM((snaps,), jnp.int32),
            pltpu.VMEM((3, (snaps + half + 1) * PITCH, LANES), f32),
            pltpu.VMEM((snaps * snaps, GROUPS * LANES), bf16),
            pltpu.VMEM((CORES, SHELLS, GROUPS * LANES), bf16),
            pltpu.VMEM((snaps * snaps, SHELLS), f32),
            pltpu.VMEM((snaps, snaps, SHELLS), f32),
            pltpu.VMEM((x_n, snaps, SHELLS), f32),
            pltpu.VMEM((snaps, SHELLS), f32),
            pltpu.VMEM((z_hi_n, snaps, SHELLS), f32),
            pltpu.VMEM((snaps, 2, 2, SHELLS), f32),
            pltpu.VMEM((z_hi_n, snaps, 2, 2, SHELLS), f32),
            pltpu.VMEM((snaps, 1, SHELLS), f32),
            pltpu.VMEM((OUT_ROWS, SHELLS), f32),
            dma((4,)),
            dma((snaps,)),
            dma((CORES, snaps)),
            dma(()),
            dma(()),
            dma((snaps,)),
            dma((snaps,)),
            dma((x_n,)),
            dma((x_n,)),
            dma((heads, snaps)),
            dma((z_hi_n, snaps)),
            dma((3,)),
            dma(()),
        ],
        compiler_params=pltpu.CompilerParams(collective_id=0, has_side_effects=True),
    )(vel, ids, ref_order)
    return pl.pallas_call(
        functools.partial(finish, snaps),
        out_shape=(
            jax.ShapeDtypeStruct((1, snaps, SHELLS), f32),
            jax.ShapeDtypeStruct((1, SHELLS), f32),
        ),
        in_specs=[pl.BlockSpec(memory_space=pltpu.VMEM)],
        out_specs=(pl.BlockSpec(memory_space=pl.ANY),) * 2,
        scratch_shapes=[dma((2,))],
    )(pltpu.with_memory_space_constraint(done, pltpu.VMEM))


def solution(mesh):
    snaps, slabs = mesh.shape["tm"], mesh.shape["slab"]
    z_hi_n = min(Z_HI, slabs // CORES)
    sizes = (snaps, slabs // CORES // z_hi_n, z_hi_n)
    return jax.shard_map(
        functools.partial(body, sizes),
        mesh=mesh,
        in_specs=(P("tm", None, None, "slab"), P("slab"), P()),
        out_specs=(P("tm", None, None), P("tm", None)),
        check_vma=False,
    )
```

```python
import functools

import jax
import jax.numpy as jnp
from jax import lax
from jax.experimental import pallas as pl
from jax.experimental.pallas import tpu as pltpu
from jax.sharding import PartitionSpec as P

SHELLS = 128
LANES = 128
Z_LO, Z_HI, CORES = 2, 4, 2
ROWS = 16
GROUPS = ROWS // 2
PITCH = ROWS + 1
OUT_ROWS = 24


def remote(src, dst, send_sem, recv_sem, tm, slab):
    return pltpu.make_async_remote_copy(
        src_ref=src,
        dst_ref=dst,
        send_sem=send_sem,
        recv_sem=recv_sem,
        device_id={"tm": tm, "slab": slab},
        device_id_type=pl.DeviceIdType.MESH,
    )


def arrived(ref, sem):
    remote(ref, ref, sem, sem, lax.axis_index("tm"), lax.axis_index("slab")).wait_recv()


def left(ref, sem):
    remote(ref, ref, sem, sem, lax.axis_index("tm"), lax.axis_index("slab")).wait_send()


def ordered_sum(terms):
    total = terms[0]
    for term in terms[1:]:
        total = total + term
    return total


def kernel(
    sizes,
    vel_ref,
    shell_ref,
    order_hbm,
    out_ref,
    src,
    recv,
    ids,
    order_ref,
    wide,
    terms,
    onehot,
    binned,
    sums,
    r_recv,
    x_recv,
    own_src,
    own_recv,
    pair_src,
    pair_recv,
    coh_rows,
    final,
    load_sem,
    m_send,
    m_recv,
    i_send,
    i_recv,
    r_send,
    r_rsem,
    x_send,
    x_rsem,
    p_send,
    o_send,
    p_rsem,
    f_send,
    f_rsem,
):
    snaps, x_n, z_hi_n = sizes
    half = snaps // 2
    heads = min(2, z_hi_n)
    me = lax.axis_index("tm")
    slab = lax.axis_index("slab")
    core = slab % CORES
    x, z_hi = slab // CORES // z_hi_n, slab // CORES % z_hi_n
    far = slab - core
    near = far + 1
    by_distance = sorted(range(1, snaps), key=lambda d: (-min(d, snaps - d), d))

    def there(d):
        return (me + d) % snaps

    def whence(d):
        return (me + snaps - d) % snaps

    def slab_of(xx, zz, cc):
        return (xx * z_hi_n + zz) * CORES + cc

    def many(n):
        if 2 * n > vel_ref.shape[1]:
            return vel_ref.at[pl.ds(0, 2), pl.ds(0, n)]
        return vel_ref.at[0, pl.ds(0, 2 * n)]

    def rows_of(t, n):
        return pl.ds(pl.multiple_of(t * n, n), n)

    load_all = pltpu.make_async_copy(vel_ref, src, load_sem.at[0])
    load_all.start()
    load_ids = pltpu.make_async_copy(
        shell_ref.at[rows_of(me, GROUPS)], ids.at[core], load_sem.at[1]
    )
    load_own = pltpu.make_async_copy(
        vel_ref.at[:, rows_of(me, ROWS)], recv.at[1, me], m_recv.at[1]
    )
    load_order = pltpu.make_async_copy(order_hbm, order_ref, load_sem.at[2])

    barrier = pltpu.get_barrier_semaphore()

    def greet(tm, sl):
        pl.semaphore_signal(
            barrier, inc=1, device_id={"tm": tm, "slab": sl}, device_id_type=pl.DeviceIdType.MESH
        )

    with jax.named_scope("a_greet"):

        @pl.when(core == 1)
        def _():
            for d in by_distance:
                greet(there(d), near)
                greet(there(d), far)
            greet(me, far)
            for d in range(1, x_n):
                greet(there(0), slab_of((x + d) % x_n, z_hi, 1))

        load_ids.start()

        @pl.when(core == 1)
        def _():
            load_own.start()
            load_order.start()

            @pl.when(z_hi < heads)
            def _():
                for h in range(1, z_hi_n):
                    for d in range(snaps):
                        greet(there(d), slab_of(x, (z_hi + h) % z_hi_n, 1))

    with jax.named_scope("b_barrier"):

        @pl.when(core == 0)
        def _():
            pl.semaphore_wait(barrier, snaps)

        @pl.when(core == 1)
        def _():
            @pl.when(z_hi < heads)
            def _():
                pl.semaphore_wait(barrier, snaps - 1 + x_n - 1 + (heads - 1) * snaps)

            @pl.when(z_hi >= heads)
            def _():
                pl.semaphore_wait(barrier, snaps - 1 + x_n - 1 + heads * snaps)

    def part_copy(d):
        return remote(
            src.at[:, rows_of(there(d), ROWS)],
            recv.at[core, me],
            m_send,
            m_recv.at[core],
            there(d),
            near,
        )

    def ids_copy():
        return remote(ids.at[0], ids.at[0], i_send, i_recv, me, near)

    ahead = 1 if x_n > 1 else 0
    first_head = (me == 0) & (z_hi == 0)
    late = z_hi_n - 1 - z_hi

    def forward(xx, zz, c):
        remote(final, final, f_send, f_rsem, me, slab_of(xx, zz, c)).start()

    def forward_all():
        for xx in range(x_n):

            @pl.when(x == xx)
            def _(xx=xx):
                if xx or not ahead:
                    forward(xx, z_hi, 0)
                else:

                    @pl.when(jnp.logical_not(first_head))
                    def _():
                        forward(xx, z_hi, 0)

                if xx == ahead and xx:

                    @pl.when(first_head)
                    def _():
                        forward(0, z_hi, 0)

                @pl.when(late >= heads)
                def _():
                    for to in {0: () if ahead else (0,), 1: (0, 1)}.get(xx, (xx,)):
                        forward(to, late, 1)
                        forward(to, late, 0)

    def forwards_left():
        for xx in range(x_n):
            for is_first in (False, True):
                for has_late in (False, True):
                    copies = 1
                    if xx == 0 and ahead and is_first:
                        copies -= 1
                    if xx == 1 and is_first:
                        copies += 1
                    if has_late:
                        copies += 2 * len({0: () if ahead else (0,), 1: (0, 1)}.get(xx, (xx,)))
                    if copies:

                        @pl.when(
                            (x == xx)
                            & (first_head == is_first)
                            & ((late >= heads) == has_late)
                        )
                        def _(copies=copies):
                            left(many(copies * OUT_ROWS), f_send)

    load_all.wait()
    for d in by_distance:
        part_copy(d).start()

    @pl.when(core == 0)
    def _():
        part_copy(0).start()
        load_ids.wait()
        ids_copy().start()

    @pl.when(core == 1)
    def _():
        shells = lax.broadcasted_iota(jnp.int32, (SHELLS, LANES), 0)
        first = lax.broadcasted_iota(jnp.int32, (snaps, LANES), 0) < half

        def spread_shells(c):
            for g in range(GROUPS):
                row = jnp.broadcast_to(ids[c, g : g + 1, :], (SHELLS, LANES))
                hot = jnp.where(row == shells, 1.0, 0.0).astype(jnp.bfloat16)
                onehot[c, :, g * LANES : (g + 1) * LANES] = hot

        def widen(core_of):
            for t in range(snaps):
                for c in range(3):
                    value = recv[core_of, t, c].astype(jnp.float32)
                    wide[c, t * PITCH : t * PITCH + ROWS, :] = value
                    if t < half:
                        at = (t + snaps) * PITCH
                        wide[c, at : at + ROWS, :] = value

        def products(g):
            def rows(c, p, d):
                return wide[c, pl.ds(d * PITCH + 2 * g + p, snaps, stride=PITCH), :]

            def put(k, value):
                terms[k * snaps : (k + 1) * snaps, g * LANES : (g + 1) * LANES] = value.astype(
                    jnp.bfloat16
                )

            own = [[rows(c, p, 0) for p in range(2)] for c in range(3)]
            put(0, sum(own[c][p] * own[c][p] for c in range(3) for p in range(2)))
            for d in range(1, half + 1):
                other = [[rows(c, p, d) for p in range(2)] for c in range(3)]
                real = sum(own[c][p] * other[c][p] for c in range(3) for p in range(2))
                imag = sum(own[c][1] * other[c][0] - own[c][0] * other[c][1] for c in range(3))
                if d < half:
                    put(2 * d - 1, real)
                    put(2 * d, imag)
                else:
                    put(2 * d - 1, jnp.where(first, real, imag))

        def bin_part(core_of, q):
            for g in (2 * q, 2 * q + 1):
                products(g)
            modes = slice(2 * q * LANES, 2 * (q + 1) * LANES)
            return lax.dot_general(
                terms[:, modes],
                onehot[core_of, :, modes],
                (((1,), (1,)), ((), ())),
                preferred_element_type=jnp.float32,
            )

        with jax.named_scope("c_onehot"):
            load_ids.wait()
            spread_shells(1)
            ids_copy().wait_recv()
            spread_shells(0)
        with jax.named_scope("d_wait1"):
            arrived(recv.at[1], m_recv.at[1])
        with jax.named_scope("e_work1"):
            widen(1)
            binned[...] = bin_part(1, 0)
            for q in range(1, GROUPS // 2):
                binned[...] += bin_part(1, q)
        with jax.named_scope("f_wait0"):
            arrived(recv.at[0], m_recv.at[0])
        with jax.named_scope("g_work0"):
            widen(0)
            for q in range(GROUPS // 2 - 1):
                binned[...] += bin_part(0, q)
            both = binned[...] + bin_part(0, GROUPS // 2 - 1)
            for k in range(snaps):
                sums[pl.ds(k, snaps, stride=snaps), :] = both[k * snaps : (k + 1) * snaps]

        with jax.named_scope("h_owner"):
            for d in by_distance:
                remote(
                    sums.at[rows_of(there(d), snaps)],
                    r_recv.at[me],
                    r_send,
                    r_rsem,
                    there(d),
                    slab,
                ).start()
            r_recv[me] = sums[rows_of(me, snaps), :]
            arrived(r_recv.at[pl.ds(0, snaps - 1)], r_rsem)
            x_recv[x] = ordered_sum([r_recv[t] for t in range(snaps)])

        with jax.named_scope("i_x"):
            for d in range(1, x_n):
                remote(
                    x_recv.at[x],
                    x_recv.at[x],
                    x_send,
                    x_rsem,
                    me,
                    slab_of((x + d) % x_n, z_hi, 1),
                ).start()
            if x_n > 1:
                arrived(x_recv.at[pl.ds(0, x_n - 1)], x_rsem)
            total = ordered_sum([x_recv[i] for i in range(x_n)])

        with jax.named_scope("j_pairs"):
            own_src[...] = total
            for d in range(1, snaps):
                pair_src[d, 0, 0:1, :] = total[0:1]
                if d < half:
                    pair_src[d, 1, :, :] = total[2 * d - 1 : 2 * d + 1]
                elif d == half:
                    pair_src[d, 1, 0:1, :] = total[2 * d - 1 : 2 * d]
                    pair_src[d, 1, 1:2, :] = jnp.zeros((1, SHELLS), jnp.float32)
                pair_src[d, 0, 1:2, :] = jnp.zeros((1, SHELLS), jnp.float32)

        def pair_ref(ref, d):
            return ref.at[d] if d <= half else ref.at[d, 0]

        def pair_send(h, d):
            return remote(
                pair_ref(pair_src, d),
                pair_ref(pair_recv.at[z_hi], d),
                p_send,
                p_rsem,
                there(d),
                slab_of(x, h, 1),
            )

        def own_send(h):
            return remote(
                own_src,
                own_recv.at[z_hi],
                o_send,
                p_rsem,
                me,
                slab_of(x, h, 1),
            )

        with jax.named_scope("k_send"):
            for h in range(heads):
                for d in by_distance:
                    pair_send(h, d).start()

                @pl.when(z_hi != h)
                def _(h=h):
                    own_send(h).start()

                @pl.when(z_hi == h)
                def _(h=h):
                    own_recv[h] = own_src[...]

        @pl.when(z_hi < heads)
        def _():
            with jax.named_scope("l_pairwait"):
                each = 4 * half + 2 * (snaps - 1 - half)
                arrived(many(z_hi_n * each + (z_hi_n - 1) * snaps), p_rsem)

            with jax.named_scope("m_coh"):
                load_order.wait()
                own = ordered_sum([own_recv[h] for h in range(z_hi_n)])
                spec = own[0:1]
                energy = [spec] + [
                    ordered_sum([pair_recv[h, d, 0, 0:1, :] for h in range(z_hi_n)])
                    for d in range(1, snaps)
                ]
                final[snaps : snaps + 1, :] = spec
                coh_rows[0] = spec * spec / (spec * spec)
                for e in range(1, snaps):
                    if e <= half:
                        pair = ordered_sum([pair_recv[h, e, 1] for h in range(z_hi_n)])
                        re, im = pair[0:1], pair[1:2]
                        if e == half:
                            im = own[2 * e - 1 : 2 * e]
                    else:
                        d = snaps - e
                        re, im = own[2 * d - 1 : 2 * d], own[2 * d : 2 * d + 1]
                    coh_rows[e] = (re * re + im * im) / (spec * energy[e])
                for j in range(snaps):
                    final[j : j + 1, :] = coh_rows[(me - order_ref[j] + snaps) % snaps]
                forward_all()

        @pl.when(z_hi >= heads)
        def _():
            with jax.named_scope("n_finalwait"):
                arrived(final, f_rsem)
                load_order.wait()

    @pl.when(core == 0)
    def _():
        with jax.named_scope("n_finalwait"):
            arrived(final, f_rsem)

    with jax.named_scope("o_end"):
        out_ref[...] = final[0 : snaps + 1]
        @pl.when(core == 0)
        def _():
            left(src, m_send)
            left(ids.at[0], i_send)

        @pl.when(core == 1)
        def _():
            left(recv.at[1, pl.ds(0, snaps - 1)], m_send)
            left(r_recv.at[pl.ds(0, snaps - 1)], r_send)
            if x_n > 1:
                left(x_recv.at[pl.ds(0, x_n - 1)], x_send)
            left(many(heads * (4 * half + 2 * (snaps - 1 - half))), p_send)

            @pl.when(z_hi < heads)
            def _():
                if heads > 1:
                    left(own_recv.at[pl.ds(0, heads - 1)], o_send)
                forwards_left()

            @pl.when(z_hi >= heads)
            def _():
                left(own_recv.at[pl.ds(0, heads)], o_send)


def finish(snaps, done_ref, coh_ref, spec_ref, sem):
    coh = pltpu.make_async_copy(done_ref.at[0:snaps], coh_ref.at[0], sem.at[0])
    spec = pltpu.make_async_copy(done_ref.at[snaps : snaps + 1], spec_ref, sem.at[1])
    coh.start()
    spec.start()
    coh.wait()
    spec.wait()


def body(sizes, velocity, shell_index, ref_order):
    snaps, x_n, z_hi_n = sizes
    half = snaps // 2
    heads = min(2, z_hi_n)
    lanes_n = velocity.shape[3] // LANES
    vel = velocity.reshape(3, 2, lanes_n, LANES).transpose(0, 2, 1, 3)
    vel = vel.reshape(3, 2 * lanes_n, LANES)
    ids = shell_index.reshape(lanes_n, LANES)
    f32, bf16, dma = jnp.float32, jnp.bfloat16, pltpu.SemaphoreType.DMA
    done = pl.pallas_call(
        functools.partial(kernel, sizes),
        out_shape=pltpu.VMEM((snaps + 1, SHELLS), f32),
        in_specs=[pl.BlockSpec(memory_space=pl.ANY)] * 3,
        out_specs=pl.BlockSpec(memory_space=pltpu.VMEM),
        scratch_shapes=[
            pltpu.VMEM((3, 2 * lanes_n, LANES), bf16),
            pltpu.VMEM((CORES, snaps, 3, ROWS, LANES), bf16),
            pltpu.VMEM((CORES, GROUPS, LANES), jnp.int32),
            pltpu.SMEM((snaps,), jnp.int32),
            pltpu.VMEM((3, (snaps + half + 1) * PITCH, LANES), f32),
            pltpu.VMEM((snaps * snaps, GROUPS * LANES), bf16),
            pltpu.VMEM((CORES, SHELLS, GROUPS * LANES), bf16),
            pltpu.VMEM((snaps * snaps, SHELLS), f32),
            pltpu.VMEM((snaps * snaps, SHELLS), f32),
            pltpu.VMEM((snaps, snaps, SHELLS), f32),
            pltpu.VMEM((x_n, snaps, SHELLS), f32),
            pltpu.VMEM((snaps, SHELLS), f32),
            pltpu.VMEM((z_hi_n, snaps, SHELLS), f32),
            pltpu.VMEM((snaps, 2, 2, SHELLS), f32),
            pltpu.VMEM((z_hi_n, snaps, 2, 2, SHELLS), f32),
            pltpu.VMEM((snaps, 1, SHELLS), f32),
            pltpu.VMEM((OUT_ROWS, SHELLS), f32),
            dma((3,)),
            dma(()),
            dma((CORES,)),
            *[dma(())] * 11,
        ],
        compiler_params=pltpu.CompilerParams(collective_id=0, has_side_effects=True),
    )(vel, ids, ref_order)
    return pl.pallas_call(
        functools.partial(finish, snaps),
        out_shape=(
            jax.ShapeDtypeStruct((1, snaps, SHELLS), f32),
            jax.ShapeDtypeStruct((1, SHELLS), f32),
        ),
        in_specs=[pl.BlockSpec(memory_space=pltpu.VMEM)],
        out_specs=(pl.BlockSpec(memory_space=pl.ANY),) * 2,
        scratch_shapes=[dma((2,))],
    )(pltpu.with_memory_space_constraint(done, pltpu.VMEM))


def solution(mesh):
    snaps, slabs = mesh.shape["tm"], mesh.shape["slab"]
    z_hi_n = min(Z_HI, slabs // CORES)
    sizes = (snaps, slabs // CORES // z_hi_n, z_hi_n)
    return jax.shard_map(
        functools.partial(body, sizes),
        mesh=mesh,
        in_specs=(P("tm", None, None, "slab"), P("slab"), P()),
        out_specs=(P("tm", None, None), P("tm", None)),
        check_vma=False,
    )
```

```python
import functools

import jax
import jax.numpy as jnp
from jax import lax
from jax.experimental import pallas as pl
from jax.experimental.pallas import tpu as pltpu
from jax.sharding import PartitionSpec as P

SHELLS = 128
LANES = 128
Z_LO, Z_HI, CORES = 2, 4, 2
ROWS = 16
GROUPS = ROWS // 2
PITCH = ROWS + 1
HALVES = 2
PIECE = ROWS // HALVES
OUT_ROWS = 24


def remote(src, dst, send_sem, recv_sem, tm, slab):
    return pltpu.make_async_remote_copy(
        src_ref=src,
        dst_ref=dst,
        send_sem=send_sem,
        recv_sem=recv_sem,
        device_id={"tm": tm, "slab": slab},
        device_id_type=pl.DeviceIdType.MESH,
    )


def arrived(ref, sem):
    remote(ref, ref, sem, sem, lax.axis_index("tm"), lax.axis_index("slab")).wait_recv()


def left(ref, sem):
    remote(ref, ref, sem, sem, lax.axis_index("tm"), lax.axis_index("slab")).wait_send()


def ordered_sum(terms):
    total = terms[0]
    for term in terms[1:]:
        total = total + term
    return total


def kernel(
    sizes,
    vel_ref,
    shell_ref,
    order_hbm,
    out_ref,
    src,
    recv,
    all_ids,
    peer_ids,
    order_ref,
    wide,
    terms,
    onehot,
    binned,
    sums,
    r_recv,
    x_recv,
    spec_out,
    spec_peer,
    spec_x,
    spec_recv,
    own_src,
    own_recv,
    pair_src,
    pair_recv,
    spec_rows,
    coh_rows,
    final,
    load_sem,
    m_send,
    m_recv,
    i_send,
    i_recv,
    r_send,
    r_rsem,
    x_send,
    x_rsem,
    p_send,
    p_rsem,
    o_send,
    o_rsem,
    e_send,
    e_rsem,
    s_send,
    s_rsem,
    t_send,
    t_rsem,
    f_send,
    f_rsem,
):
    snaps, x_n, z_hi_n = sizes
    half = snaps // 2
    heads = min(2, z_hi_n)
    me = lax.axis_index("tm")
    slab = lax.axis_index("slab")
    core = slab % CORES
    x, z_hi = slab // CORES // z_hi_n, slab // CORES % z_hi_n
    far = slab - core
    near = far + 1
    by_distance = sorted(range(1, snaps), key=lambda d: (-min(d, snaps - d), d))

    pairs_at = {0: (1,)}
    for step in range(1, (half + 1) // 2 + 1):
        pairs_at[step] = tuple(d for d in (2 * step - 1, 2 * step) if d <= half)
    for step in range(1, half // 2 + 1):
        pairs_at[-step] = tuple(d for d in (2 * step, 2 * step + 1) if d <= half)
    steps = sorted((i for i in pairs_at if i), key=lambda i: (-abs(i), i))
    x_steps = sorted(range(1, x_n), key=lambda d: -min(d, x_n - d))
    pair_rows = sum(2 * len(pairs_at[i]) for i in steps)

    def there(d):
        return (me + d) % snaps

    def whence(d):
        return (me + snaps - d) % snaps

    def slab_of(xx, zz, cc):
        return (xx * z_hi_n + zz) * CORES + cc

    def many(n):
        if n <= r_recv.shape[1]:
            return r_recv.at[0, pl.ds(0, n)]
        if 2 * n > vel_ref.shape[1]:
            return vel_ref.at[pl.ds(0, 2), pl.ds(0, n)]
        return vel_ref.at[0, pl.ds(0, 2 * n)]

    def rows_of(t, n):
        return pl.ds(pl.multiple_of(t * n, n), n)

    load_all = pltpu.make_async_copy(vel_ref, src, load_sem.at[0])
    load_all.start()
    load_ids = pltpu.make_async_copy(shell_ref, all_ids, load_sem.at[1])
    load_ids.start()
    load_own = [
        pltpu.make_async_copy(
            vel_ref.at[:, pl.ds(pl.multiple_of(me * ROWS + n * PIECE, PIECE), PIECE)],
            recv.at[1, n, me],
            m_recv.at[1, n],
        )
        for n in range(HALVES)
    ]
    load_order = pltpu.make_async_copy(order_hbm, order_ref, load_sem.at[2])

    barrier = pltpu.get_barrier_semaphore()

    def greet(tm, sl):
        pl.semaphore_signal(
            barrier, inc=1, device_id={"tm": tm, "slab": sl}, device_id_type=pl.DeviceIdType.MESH
        )

    with jax.named_scope("a_greet"):

        @pl.when(core == 1)
        def _():
            for d in by_distance:
                greet(there(d), near)
                greet(there(d), far)
            greet(me, far)
            for d in range(1, x_n):
                greet(there(0), slab_of((x + d) % x_n, z_hi, 1))

        @pl.when(core == 1)
        def _():
            for copy in load_own:
                copy.start()
            load_order.start()

            @pl.when(z_hi < heads)
            def _():
                for h in range(1, z_hi_n):
                    for i in pairs_at:
                        greet((me + snaps - i) % snaps, slab_of(x, (z_hi + h) % z_hi_n, 1))

    with jax.named_scope("b_barrier"):

        @pl.when(core == 0)
        def _():
            pl.semaphore_wait(barrier, snaps)

        @pl.when(core == 1)
        def _():
            @pl.when(z_hi < heads)
            def _():
                pl.semaphore_wait(barrier, snaps - 1 + x_n - 1 + (heads - 1) * len(pairs_at))

            @pl.when(z_hi >= heads)
            def _():
                pl.semaphore_wait(barrier, snaps - 1 + x_n - 1 + heads * len(pairs_at))

    def part_copy(n, d):
        return remote(
            src.at[:, pl.ds(pl.multiple_of(there(d) * ROWS + n * PIECE, PIECE), PIECE)],
            recv.at[core, n, me],
            m_send,
            m_recv.at[core, n],
            there(d),
            near,
        )

    def ids_copy():
        return remote(all_ids.at[rows_of(me, GROUPS)], peer_ids, i_send, i_recv, me, near)

    def spec_copy():
        return remote(spec_out, spec_peer, e_send, e_rsem, me, near)

    shells = lax.broadcasted_iota(jnp.int32, (SHELLS, LANES), 0)

    def local_spectrum():
        lanes_n = shell_ref.shape[0]
        squares = ordered_sum([src[c].astype(jnp.float32) ** 2 for c in range(3)])
        wide[0, 0 : 2 * lanes_n, :] = squares
        energy = wide[0, pl.ds(0, lanes_n, stride=2), :] + wide[0, pl.ds(1, lanes_n, stride=2), :]
        wide[1, 0:lanes_n, :] = energy.astype(jnp.bfloat16).astype(jnp.float32)

        def add_rows(i, total):
            at = rows_of(i, 8)
            shell, value = all_ids[at, :], wide[1, at, :]
            for r in range(8):
                hit = jnp.broadcast_to(shell[r : r + 1], (SHELLS, LANES)) == shells
                total = total + jnp.where(
                    hit, jnp.broadcast_to(value[r : r + 1], (SHELLS, LANES)), 0.0
                )
            return total

        by_lane = lax.fori_loop(
            0, lanes_n // 8, add_rows, jnp.zeros((SHELLS, LANES), jnp.float32)
        )
        return lax.dot_general(
            jnp.ones((8, LANES), jnp.float32),
            by_lane,
            (((1,), (1,)), ((), ())),
            precision=lax.Precision.HIGHEST,
            preferred_element_type=jnp.float32,
        )[0:1]

    ahead = 1 if x_n > 1 else 0
    first_head = (me == 0) & (z_hi == 0)
    late = z_hi_n - 1 - z_hi

    def forward(xx, zz, c):
        remote(final, final, f_send, f_rsem, me, slab_of(xx, zz, c)).start()

    def forward_all():
        for xx in range(x_n):

            @pl.when(x == xx)
            def _(xx=xx):
                if xx or not ahead:
                    forward(xx, z_hi, 0)
                else:

                    @pl.when(jnp.logical_not(first_head))
                    def _():
                        forward(xx, z_hi, 0)

                if xx == ahead and xx:

                    @pl.when(first_head)
                    def _():
                        forward(0, z_hi, 0)

                @pl.when(late >= heads)
                def _():
                    for to in {0: () if ahead else (0,), 1: (0, 1)}.get(xx, (xx,)):
                        forward(to, late, 1)
                        forward(to, late, 0)

    def forwards_left():
        for xx in range(x_n):
            for is_first in (False, True):
                for has_late in (False, True):
                    copies = 1
                    if xx == 0 and ahead and is_first:
                        copies -= 1
                    if xx == 1 and is_first:
                        copies += 1
                    if has_late:
                        copies += 2 * len({0: () if ahead else (0,), 1: (0, 1)}.get(xx, (xx,)))
                    if copies:

                        @pl.when(
                            (x == xx)
                            & (first_head == is_first)
                            & ((late >= heads) == has_late)
                        )
                        def _(copies=copies):
                            left(many(copies * OUT_ROWS), f_send)

    load_all.wait()

    @pl.when(core == 0)
    def _():
        for n in range(HALVES):
            for d in [*by_distance, 0]:
                part_copy(n, d).start()
        load_ids.wait()
        ids_copy().start()
        spec_out[...] = local_spectrum()
        spec_copy().start()

    @pl.when(core == 1)
    def _():
        for n in range(HALVES):
            for d in by_distance:
                part_copy(n, d).start()

        first = lax.broadcasted_iota(jnp.int32, (snaps, LANES), 0) < half

        def spread_shells(c):
            for g in range(GROUPS):
                row = all_ids[pl.ds(me * GROUPS + g, 1), :] if c else peer_ids[g : g + 1, :]
                row = jnp.broadcast_to(row, (SHELLS, LANES))
                hot = jnp.where(row == shells, 1.0, 0.0).astype(jnp.bfloat16)
                onehot[c, :, g * LANES : (g + 1) * LANES] = hot

        def widen(core_of, n):
            for t in range(snaps):
                for c in range(3):
                    value = recv[core_of, n, t, c].astype(jnp.float32)
                    for at in (t, t + snaps) if t < half else (t,):
                        row = at * PITCH + n * PIECE
                        wide[c, row : row + PIECE, :] = value

        def products(g):
            def rows(c, p, d):
                return wide[c, pl.ds(d * PITCH + 2 * g + p, snaps, stride=PITCH), :]

            def put(k, value):
                terms[k * snaps : (k + 1) * snaps, g * LANES : (g + 1) * LANES] = value.astype(
                    jnp.bfloat16
                )

            own = [[rows(c, p, 0) for p in range(2)] for c in range(3)]
            for d in range(1, half + 1):
                other = [[rows(c, p, d) for p in range(2)] for c in range(3)]
                real = sum(own[c][p] * other[c][p] for c in range(3) for p in range(2))
                imag = sum(own[c][1] * other[c][0] - own[c][0] * other[c][1] for c in range(3))
                if d < half:
                    put(2 * d - 2, real)
                    put(2 * d - 1, imag)
                else:
                    put(2 * d - 2, jnp.where(first, real, imag))

        def bin_part(core_of, q):
            for g in (2 * q, 2 * q + 1):
                products(g)
            modes = slice(2 * q * LANES, 2 * (q + 1) * LANES)
            return lax.dot_general(
                terms[:, modes],
                onehot[core_of, :, modes],
                (((1,), (1,)), ((), ())),
                preferred_element_type=jnp.float32,
            )

        with jax.named_scope("c_onehot"):
            load_ids.wait()
            spread_shells(1)
            ids_copy().wait_recv()
            spread_shells(0)
        with jax.named_scope("c_spectrum"):
            mine = local_spectrum()
            spec_copy().wait_recv()
            spec_x[x] = mine + spec_peer[...]
            for d in x_steps:
                remote(
                    spec_x.at[x],
                    spec_x.at[x],
                    t_send,
                    t_rsem,
                    me,
                    slab_of((x + d) % x_n, z_hi, 1),
                ).start()

        quarters = GROUPS // 2 // HALVES
        for n in range(HALVES):
            for c in (1, 0):
                with jax.named_scope(f"d_wait{n}{c}"):
                    arrived(recv.at[c, n], m_recv.at[c, n])
                with jax.named_scope(f"e_work{n}{c}"):
                    widen(c, n)
                    for q in range(n * quarters, (n + 1) * quarters):
                        if (n, c) == (HALVES - 1, 0) and q == (n + 1) * quarters - 1:
                            both = binned[...] + bin_part(c, q)
                        elif (n, c, q) == (0, 1, 0):
                            binned[...] = bin_part(c, q)
                        else:
                            binned[...] += bin_part(c, q)
        with jax.named_scope("g_turn"):
            for k in range(snaps - 1):
                value, shift = both[k * snaps : (k + 1) * snaps], (k // 2 + 1) // 2
                sums[pl.ds(shift * snaps + k, snaps - shift, stride=snaps), :] = value[
                    0 : snaps - shift
                ]
                if shift:
                    sums[pl.ds(k, shift, stride=snaps), :] = value[snaps - shift :]
            sums[pl.ds(snaps - 1, snaps, stride=snaps), :] = jnp.zeros((snaps, SHELLS), jnp.float32)

        with jax.named_scope("h_owner"):
            for d in by_distance:
                remote(
                    sums.at[rows_of(there(d), snaps)],
                    r_recv.at[me],
                    r_send,
                    r_rsem,
                    there(d),
                    slab,
                ).start()
            r_recv[me] = sums[rows_of(me, snaps), :]
            if x_n > 1:
                arrived(spec_x.at[pl.ds(0, x_n - 1)], t_rsem)
            spec_recv[me] = ordered_sum([spec_x[i] for i in range(x_n)])
            for d in by_distance:
                remote(
                    spec_recv.at[me], spec_recv.at[me], s_send, s_rsem, there(d), slab
                ).start()
            arrived(r_recv.at[pl.ds(0, snaps - 1)], r_rsem)
            x_recv[x] = ordered_sum([r_recv[t] for t in range(snaps)])

        with jax.named_scope("i_x"):
            for d in x_steps:
                remote(
                    x_recv.at[x],
                    x_recv.at[x],
                    x_send,
                    x_rsem,
                    me,
                    slab_of((x + d) % x_n, z_hi, 1),
                ).start()
            if x_n > 1:
                arrived(x_recv.at[pl.ds(0, x_n - 1)], x_rsem)
            total = ordered_sum([x_recv[i] for i in range(x_n)])
            arrived(spec_recv.at[pl.ds(0, snaps - 1)], s_rsem)

        with jax.named_scope("j_pairs"):
            own_src[0:snaps, :] = total
            for t in range(snaps):
                own_src[snaps + t : snaps + t + 1, :] = spec_recv[t]
            for d in range(1, half + 1):
                pair_src[d - 1] = total[2 * d - 2 : 2 * d]

        with jax.named_scope("k_send"):
            for h in range(heads):
                for i in steps:
                    count = len(pairs_at[i])
                    remote(
                        pair_src.at[pl.ds(pairs_at[i][0] - 1, count)],
                        pair_recv.at[z_hi, steps.index(i), pl.ds(0, count)],
                        p_send,
                        p_rsem,
                        (me + snaps + i) % snaps,
                        slab_of(x, h, 1),
                    ).start()

                @pl.when(z_hi != h)
                def _(h=h):
                    remote(
                        own_src, own_recv.at[z_hi], o_send, o_rsem, me, slab_of(x, h, 1)
                    ).start()

                @pl.when(z_hi == h)
                def _(h=h):
                    own_recv[h] = own_src[...]

        @pl.when(z_hi < heads)
        def _():
            with jax.named_scope("l_pairwait"):
                arrived(many(z_hi_n * pair_rows), p_rsem)
                if z_hi_n > 1:
                    arrived(own_recv.at[pl.ds(0, z_hi_n - 1)], o_rsem)

            with jax.named_scope("m_coh"):
                load_order.wait()
                own = ordered_sum([own_recv[h] for h in range(z_hi_n)])
                energy = own[snaps : 2 * snaps]
                for t in range(snaps):
                    spec_rows[t] = energy[t : t + 1]
                spec = spec_rows[me]
                final[snaps : snaps + 1, :] = spec

                def pair(i, d):
                    if i == 0:
                        return own[2 * d - 2 : 2 * d]
                    at = pairs_at[i].index(d)
                    return ordered_sum(
                        [pair_recv[h, steps.index(i), at] for h in range(z_hi_n)]
                    )

                def power(rows):
                    re, im = rows[0:1], rows[1:2]
                    return re * re + im * im

                def put_row(e, value):
                    coh_rows[e] = value / (spec * spec_rows[(me + snaps - e) % snaps])

                put_row(0, spec * spec)
                for d in range(1, half):
                    put_row(d, power(pair((d + 1) // 2, d)))
                    put_row(snaps - d, power(pair(-(d // 2), d)))
                re = pair((half + 1) // 2, half)[0:1]
                im = pair(-(half // 2), half)[0:1]
                put_row(half, re * re + im * im)
                for j in range(snaps):
                    final[j : j + 1, :] = coh_rows[(me - order_ref[j] + snaps) % snaps]
                forward_all()

        @pl.when(z_hi >= heads)
        def _():
            with jax.named_scope("n_finalwait"):
                arrived(final, f_rsem)
                load_order.wait()

    @pl.when(core == 0)
    def _():
        with jax.named_scope("n_finalwait"):
            arrived(final, f_rsem)

    with jax.named_scope("o_end"):
        out_ref[...] = final[0 : snaps + 1]
        @pl.when(core == 0)
        def _():
            left(src, m_send)
            left(peer_ids, i_send)
            left(spec_out, e_send)

        @pl.when(core == 1)
        def _():
            left(src.at[:, pl.ds(0, (snaps - 1) * ROWS)], m_send)
            left(r_recv.at[pl.ds(0, snaps - 1)], r_send)
            if x_n > 1:
                left(x_recv.at[pl.ds(0, x_n - 1)], x_send)
                left(spec_x.at[pl.ds(0, x_n - 1)], t_send)
            left(spec_recv.at[pl.ds(0, snaps - 1)], s_send)
            left(many(heads * pair_rows), p_send)

            @pl.when(z_hi < heads)
            def _():
                if heads > 1:
                    left(own_recv.at[pl.ds(0, heads - 1)], o_send)
                forwards_left()

            @pl.when(z_hi >= heads)
            def _():
                left(own_recv.at[pl.ds(0, heads)], o_send)


def finish(snaps, done_ref, coh_ref, spec_ref, sem):
    coh = pltpu.make_async_copy(done_ref.at[0:snaps], coh_ref.at[0], sem.at[0])
    spec = pltpu.make_async_copy(done_ref.at[snaps : snaps + 1], spec_ref, sem.at[1])
    coh.start()
    spec.start()
    coh.wait()
    spec.wait()


def body(sizes, velocity, shell_index, ref_order):
    snaps, x_n, z_hi_n = sizes
    half = snaps // 2
    heads = min(2, z_hi_n)
    lanes_n = velocity.shape[3] // LANES
    vel = velocity.reshape(3, 2, lanes_n, LANES).transpose(0, 2, 1, 3)
    vel = vel.reshape(3, 2 * lanes_n, LANES)
    ids = shell_index.reshape(lanes_n, LANES)
    f32, bf16, dma = jnp.float32, jnp.bfloat16, pltpu.SemaphoreType.DMA
    done = pl.pallas_call(
        functools.partial(kernel, sizes),
        out_shape=pltpu.VMEM((snaps + 1, SHELLS), f32),
        in_specs=[pl.BlockSpec(memory_space=pl.ANY)] * 3,
        out_specs=pl.BlockSpec(memory_space=pltpu.VMEM),
        scratch_shapes=[
            pltpu.VMEM((3, 2 * lanes_n, LANES), bf16),
            pltpu.VMEM((CORES, HALVES, snaps, 3, PIECE, LANES), bf16),
            pltpu.VMEM((lanes_n, LANES), jnp.int32),
            pltpu.VMEM((GROUPS, LANES), jnp.int32),
            pltpu.SMEM((snaps,), jnp.int32),
            pltpu.VMEM((3, (snaps + half + 1) * PITCH, LANES), f32),
            pltpu.VMEM(((snaps - 1) * snaps, GROUPS * LANES), bf16),
            pltpu.VMEM((CORES, SHELLS, GROUPS * LANES), bf16),
            pltpu.VMEM(((snaps - 1) * snaps, SHELLS), f32),
            pltpu.VMEM((snaps * snaps, SHELLS), f32),
            pltpu.VMEM((snaps, snaps, SHELLS), f32),
            pltpu.VMEM((x_n, snaps, SHELLS), f32),
            pltpu.VMEM((1, SHELLS), f32),
            pltpu.VMEM((1, SHELLS), f32),
            pltpu.VMEM((x_n, 1, SHELLS), f32),
            pltpu.VMEM((snaps, 1, SHELLS), f32),
            pltpu.VMEM((2 * snaps, SHELLS), f32),
            pltpu.VMEM((z_hi_n, 2 * snaps, SHELLS), f32),
            pltpu.VMEM((half, 2, SHELLS), f32),
            pltpu.VMEM((z_hi_n, half, 2, 2, SHELLS), f32),
            pltpu.VMEM((snaps, 1, SHELLS), f32),
            pltpu.VMEM((snaps, 1, SHELLS), f32),
            pltpu.VMEM((OUT_ROWS, SHELLS), f32),
            dma((3,)),
            dma(()),
            dma((CORES, HALVES)),
            *[dma(())] * 18,
        ],
        compiler_params=pltpu.CompilerParams(collective_id=0, has_side_effects=True),
    )(vel, ids, ref_order)
    return pl.pallas_call(
        functools.partial(finish, snaps),
        out_shape=(
            jax.ShapeDtypeStruct((1, snaps, SHELLS), f32),
            jax.ShapeDtypeStruct((1, SHELLS), f32),
        ),
        in_specs=[pl.BlockSpec(memory_space=pltpu.VMEM)],
        out_specs=(pl.BlockSpec(memory_space=pl.ANY),) * 2,
        scratch_shapes=[dma((2,))],
    )(pltpu.with_memory_space_constraint(done, pltpu.VMEM))


def solution(mesh):
    snaps, slabs = mesh.shape["tm"], mesh.shape["slab"]
    z_hi_n = min(Z_HI, slabs // CORES)
    sizes = (snaps, slabs // CORES // z_hi_n, z_hi_n)
    return jax.shard_map(
        functools.partial(body, sizes),
        mesh=mesh,
        in_specs=(P("tm", None, None, "slab"), P("slab"), P()),
        out_specs=(P("tm", None, None), P("tm", None)),
        check_vma=False,
    )
```

```python
import functools

import jax
import jax.numpy as jnp
from jax import lax
from jax.experimental import pallas as pl
from jax.experimental.pallas import tpu as pltpu
from jax.sharding import PartitionSpec as P

SHELLS = 128
LANES = 128
Z_LO, Z_HI, CORES = 2, 4, 2
ROWS = 16
GROUPS = ROWS // 2
PITCH = ROWS + 1
SETS = 3
HALVES = 2
PIECE = ROWS // HALVES
OUT_ROWS = 24


def remote(src, dst, send_sem, recv_sem, tm, slab):
    return pltpu.make_async_remote_copy(
        src_ref=src,
        dst_ref=dst,
        send_sem=send_sem,
        recv_sem=recv_sem,
        device_id={"tm": tm, "slab": slab},
        device_id_type=pl.DeviceIdType.MESH,
    )


def arrived(ref, sem):
    remote(ref, ref, sem, sem, lax.axis_index("tm"), lax.axis_index("slab")).wait_recv()


def left(ref, sem):
    remote(ref, ref, sem, sem, lax.axis_index("tm"), lax.axis_index("slab")).wait_send()


def ordered_sum(terms):
    total = terms[0]
    for term in terms[1:]:
        total = total + term
    return total


def kernel(
    sizes,
    vel_ref,
    shell_ref,
    order_hbm,
    out_ref,
    src,
    recv,
    all_ids,
    peer_ids,
    order_ref,
    wide,
    terms,
    onehot,
    binned,
    sums,
    r_recv,
    x_recv,
    spec_out,
    spec_peer,
    spec_x,
    spec_recv,
    own_src,
    own_recv,
    pair_src,
    pair_recv,
    spec_rows,
    coh_rows,
    final,
    load_sem,
    m_send,
    m_recv,
    i_send,
    i_recv,
    r_send,
    r_rsem,
    x_send,
    x_rsem,
    p_send,
    p_rsem,
    o_send,
    o_rsem,
    e_send,
    e_rsem,
    s_send,
    s_rsem,
    t_send,
    t_rsem,
    f_send,
    f_rsem,
):
    snaps, x_n, z_hi_n = sizes
    half = snaps // 2
    heads = min(2, z_hi_n)
    me = lax.axis_index("tm")
    slab = lax.axis_index("slab")
    core = slab % CORES
    x, z_hi = slab // CORES // z_hi_n, slab // CORES % z_hi_n
    far = slab - core
    near = far + 1
    late = z_hi_n - 1 - z_hi
    is_late = z_hi // heads
    part_set = core + (1 - core) * 2 * is_late
    by_distance = sorted(range(1, snaps), key=lambda d: (-min(d, snaps - d), d))

    pairs_at = {0: (1,)}
    for step in range(1, (half + 1) // 2 + 1):
        pairs_at[step] = tuple(d for d in (2 * step - 1, 2 * step) if d <= half)
    for step in range(1, half // 2 + 1):
        pairs_at[-step] = tuple(d for d in (2 * step, 2 * step + 1) if d <= half)
    steps = sorted((i for i in pairs_at if i), key=lambda i: (-abs(i), i))
    x_steps = sorted(range(1, x_n), key=lambda d: -min(d, x_n - d))
    pair_rows = sum(2 * len(pairs_at[i]) for i in steps)

    def there(d):
        return (me + d) % snaps

    def whence(d):
        return (me + snaps - d) % snaps

    def slab_of(xx, zz, cc):
        return (xx * z_hi_n + zz) * CORES + cc

    def many(n):
        if n <= r_recv.shape[1]:
            return r_recv.at[0, pl.ds(0, n)]
        if 2 * n > vel_ref.shape[1]:
            return vel_ref.at[pl.ds(0, 2), pl.ds(0, n)]
        return vel_ref.at[0, pl.ds(0, 2 * n)]

    def rows_of(t, n):
        return pl.ds(pl.multiple_of(t * n, n), n)

    load_all = pltpu.make_async_copy(vel_ref, src, load_sem.at[0])
    load_all.start()
    load_ids = pltpu.make_async_copy(shell_ref, all_ids, load_sem.at[1])
    load_ids.start()
    load_own = [
        pltpu.make_async_copy(
            vel_ref.at[:, pl.ds(pl.multiple_of(me * ROWS + n * PIECE, PIECE), PIECE)],
            recv.at[1, n, me],
            m_recv.at[1, n],
        )
        for n in range(HALVES)
    ]
    load_order = pltpu.make_async_copy(order_hbm, order_ref, load_sem.at[2])

    barrier = pltpu.get_barrier_semaphore()

    def greet(tm, sl):
        pl.semaphore_signal(
            barrier, inc=1, device_id={"tm": tm, "slab": sl}, device_id_type=pl.DeviceIdType.MESH
        )

    with jax.named_scope("a_greet"):

        @pl.when(core == 1)
        def _():
            @pl.when(z_hi < heads)
            def _():
                @pl.when(late >= heads)
                def _():
                    for d in [*by_distance, 0]:
                        greet(there(d), slab_of(x, late, 0))

                for d in by_distance:
                    greet(there(d), near)
                    greet(there(d), far)

            @pl.when(z_hi >= heads)
            def _():
                for d in by_distance:
                    greet(there(d), near)

            greet(me, far)
            for d in range(1, x_n):
                greet(there(0), slab_of((x + d) % x_n, z_hi, 1))

        @pl.when(core == 1)
        def _():
            for copy in load_own:
                copy.start()
            load_order.start()

            @pl.when(z_hi < heads)
            def _():
                for h in range(1, z_hi_n):
                    for i in pairs_at:
                        greet((me + snaps - i) % snaps, slab_of(x, (z_hi + h) % z_hi_n, 1))

    with jax.named_scope("b_barrier"):

        @pl.when(core == 0)
        def _():
            @pl.when(z_hi < heads)
            def _():
                pl.semaphore_wait(barrier, snaps)

            @pl.when(z_hi >= heads)
            def _():
                pl.semaphore_wait(barrier, snaps + 1)

        @pl.when(core == 1)
        def _():
            @pl.when(z_hi < heads)
            def _():
                pl.semaphore_wait(barrier, snaps - 1 + x_n - 1 + (heads - 1) * len(pairs_at))

            @pl.when(z_hi >= heads)
            def _():
                pl.semaphore_wait(barrier, snaps - 1 + x_n - 1 + heads * len(pairs_at))

    def part_copy(n, d):
        return remote(
            src.at[:, pl.ds(pl.multiple_of(there(d) * ROWS + n * PIECE, PIECE), PIECE)],
            recv.at[part_set, n, me],
            m_send,
            m_recv.at[part_set, n],
            there(d),
            slab_of(x, z_hi + (1 - core) * is_late * (late - z_hi), 1),
        )

    def ids_copy():
        return remote(
            all_ids.at[rows_of(me, GROUPS)],
            peer_ids.at[is_late],
            i_send,
            i_recv.at[is_late],
            me,
            slab_of(x, z_hi + is_late * (late - z_hi), 1),
        )

    def spec_copy():
        return remote(spec_out, spec_peer, e_send, e_rsem, me, near)

    shells = lax.broadcasted_iota(jnp.int32, (SHELLS, LANES), 0)

    def local_spectrum():
        lanes_n = shell_ref.shape[0]
        squares = ordered_sum([src[c].astype(jnp.float32) ** 2 for c in range(3)])
        wide[0, 0 : 2 * lanes_n, :] = squares
        energy = wide[0, pl.ds(0, lanes_n, stride=2), :] + wide[0, pl.ds(1, lanes_n, stride=2), :]
        wide[1, 0:lanes_n, :] = energy.astype(jnp.bfloat16).astype(jnp.float32)

        def add_rows(i, total):
            at = rows_of(i, 8)
            shell, value = all_ids[at, :], wide[1, at, :]
            for r in range(8):
                hit = jnp.broadcast_to(shell[r : r + 1], (SHELLS, LANES)) == shells
                total = total + jnp.where(
                    hit, jnp.broadcast_to(value[r : r + 1], (SHELLS, LANES)), 0.0
                )
            return total

        by_lane = lax.fori_loop(
            0, lanes_n // 8, add_rows, jnp.zeros((SHELLS, LANES), jnp.float32)
        )
        return lax.dot_general(
            jnp.ones((8, LANES), jnp.float32),
            by_lane,
            (((1,), (1,)), ((), ())),
            precision=lax.Precision.HIGHEST,
            preferred_element_type=jnp.float32,
        )[0:1]

    ahead = 1 if x_n > 1 else 0
    first_head = (me == 0) & (z_hi == 0)

    def forward(xx, zz, c):
        remote(final, final, f_send, f_rsem, me, slab_of(xx, zz, c)).start()

    def forward_all():
        for xx in range(x_n):

            @pl.when(x == xx)
            def _(xx=xx):
                if xx or not ahead:
                    forward(xx, z_hi, 0)
                else:

                    @pl.when(jnp.logical_not(first_head))
                    def _():
                        forward(xx, z_hi, 0)

                if xx == ahead and xx:

                    @pl.when(first_head)
                    def _():
                        forward(0, z_hi, 0)

                @pl.when(late >= heads)
                def _():
                    for to in {0: () if ahead else (0,), 1: (0, 1)}.get(xx, (xx,)):
                        forward(to, late, 1)
                        forward(to, late, 0)

    def forwards_left():
        for xx in range(x_n):
            for is_first in (False, True):
                for has_late in (False, True):
                    copies = 1
                    if xx == 0 and ahead and is_first:
                        copies -= 1
                    if xx == 1 and is_first:
                        copies += 1
                    if has_late:
                        copies += 2 * len({0: () if ahead else (0,), 1: (0, 1)}.get(xx, (xx,)))
                    if copies:

                        @pl.when(
                            (x == xx)
                            & (first_head == is_first)
                            & ((late >= heads) == has_late)
                        )
                        def _(copies=copies):
                            left(many(copies * OUT_ROWS), f_send)

    load_all.wait()

    @pl.when(core == 0)
    def _():
        for n in range(HALVES):
            for d in [*by_distance, 0]:
                part_copy(n, d).start()
        load_ids.wait()
        ids_copy().start()
        spec_out[...] = local_spectrum()
        spec_copy().start()

    @pl.when(core == 1)
    def _():
        for n in range(HALVES):
            for d in by_distance:
                part_copy(n, d).start()

        first = lax.broadcasted_iota(jnp.int32, (snaps, LANES), 0) < half

        def spread_shells(c):
            for g in range(GROUPS):
                if c == 1:
                    row = all_ids[pl.ds(me * GROUPS + g, 1), :]
                else:
                    row = peer_ids[c // 2, g : g + 1, :]
                row = jnp.broadcast_to(row, (SHELLS, LANES))
                hot = jnp.where(row == shells, 1.0, 0.0).astype(jnp.bfloat16)
                onehot[c, :, g * LANES : (g + 1) * LANES] = hot

        def widen(core_of, n):
            for t in range(snaps):
                for c in range(3):
                    value = recv[core_of, n, t, c].astype(jnp.float32)
                    for at in (t, t + snaps) if t < half else (t,):
                        row = at * PITCH + n * PIECE
                        wide[c, row : row + PIECE, :] = value

        def products(g):
            def rows(c, p, d):
                return wide[c, pl.ds(d * PITCH + 2 * g + p, snaps, stride=PITCH), :]

            def put(k, value):
                terms[k * snaps : (k + 1) * snaps, g * LANES : (g + 1) * LANES] = value.astype(
                    jnp.bfloat16
                )

            own = [[rows(c, p, 0) for p in range(2)] for c in range(3)]
            for d in range(1, half + 1):
                other = [[rows(c, p, d) for p in range(2)] for c in range(3)]
                real = sum(own[c][p] * other[c][p] for c in range(3) for p in range(2))
                imag = sum(own[c][1] * other[c][0] - own[c][0] * other[c][1] for c in range(3))
                if d < half:
                    put(2 * d - 2, real)
                    put(2 * d - 1, imag)
                else:
                    put(2 * d - 2, jnp.where(first, real, imag))

        def bin_part(core_of, q):
            for g in (2 * q, 2 * q + 1):
                products(g)
            modes = slice(2 * q * LANES, 2 * (q + 1) * LANES)
            return lax.dot_general(
                terms[:, modes],
                onehot[core_of, :, modes],
                (((1,), (1,)), ((), ())),
                preferred_element_type=jnp.float32,
            )

        with jax.named_scope("c_onehot"):
            load_ids.wait()
            spread_shells(1)

            @pl.when(z_hi < heads)
            def _():
                arrived(peer_ids.at[0], i_recv.at[0])
                spread_shells(0)

        with jax.named_scope("c_spectrum"):
            mine = local_spectrum()
            spec_copy().wait_recv()
            spec_x[x] = mine + spec_peer[...]
            for d in x_steps:
                remote(
                    spec_x.at[x],
                    spec_x.at[x],
                    t_send,
                    t_rsem,
                    me,
                    slab_of((x + d) % x_n, z_hi, 1),
                ).start()

        quarters = GROUPS // 2 // HALVES

        def work_off(c, n):
            with jax.named_scope(f"d_wait{c}{n}"):
                arrived(recv.at[c, n], m_recv.at[c, n])
            with jax.named_scope(f"e_work{c}{n}"):
                widen(c, n)
                for q in range(n * quarters, (n + 1) * quarters):
                    if (c, q) == (1, 0):
                        binned[...] = bin_part(c, q)
                    else:
                        binned[...] += bin_part(c, q)

        for n in range(HALVES):
            work_off(1, n)

            @pl.when(z_hi < heads)
            def _(n=n):
                work_off(0, n)

        @pl.when((z_hi < heads) & (late >= heads))
        def _():
            arrived(peer_ids.at[1], i_recv.at[1])
            spread_shells(2)
            for n in range(HALVES):
                work_off(2, n)

        with jax.named_scope("g_turn"):
            for k in range(snaps - 1):
                value, shift = binned[k * snaps : (k + 1) * snaps], (k // 2 + 1) // 2
                sums[pl.ds(shift * snaps + k, snaps - shift, stride=snaps), :] = value[
                    0 : snaps - shift
                ]
                if shift:
                    sums[pl.ds(k, shift, stride=snaps), :] = value[snaps - shift :]
            sums[pl.ds(snaps - 1, snaps, stride=snaps), :] = jnp.zeros((snaps, SHELLS), jnp.float32)

        with jax.named_scope("h_owner"):
            for d in by_distance:
                remote(
                    sums.at[rows_of(there(d), snaps)],
                    r_recv.at[me],
                    r_send,
                    r_rsem,
                    there(d),
                    slab,
                ).start()
            r_recv[me] = sums[rows_of(me, snaps), :]
            if x_n > 1:
                arrived(spec_x.at[pl.ds(0, x_n - 1)], t_rsem)
            spec_recv[me] = ordered_sum([spec_x[i] for i in range(x_n)])
            for d in by_distance:
                remote(
                    spec_recv.at[me], spec_recv.at[me], s_send, s_rsem, there(d), slab
                ).start()
            arrived(r_recv.at[pl.ds(0, snaps - 1)], r_rsem)
            x_recv[x] = ordered_sum([r_recv[t] for t in range(snaps)])

        with jax.named_scope("i_x"):
            for d in x_steps:
                remote(
                    x_recv.at[x],
                    x_recv.at[x],
                    x_send,
                    x_rsem,
                    me,
                    slab_of((x + d) % x_n, z_hi, 1),
                ).start()
            if x_n > 1:
                arrived(x_recv.at[pl.ds(0, x_n - 1)], x_rsem)
            total = ordered_sum([x_recv[i] for i in range(x_n)])
            arrived(spec_recv.at[pl.ds(0, snaps - 1)], s_rsem)

        with jax.named_scope("j_pairs"):
            own_src[0:snaps, :] = total
            for t in range(snaps):
                own_src[snaps + t : snaps + t + 1, :] = spec_recv[t]
            for d in range(1, half + 1):
                pair_src[d - 1] = total[2 * d - 2 : 2 * d]

        with jax.named_scope("k_send"):
            for h in range(heads):
                for i in steps:
                    count = len(pairs_at[i])
                    remote(
                        pair_src.at[pl.ds(pairs_at[i][0] - 1, count)],
                        pair_recv.at[z_hi, steps.index(i), pl.ds(0, count)],
                        p_send,
                        p_rsem,
                        (me + snaps + i) % snaps,
                        slab_of(x, h, 1),
                    ).start()

                @pl.when(z_hi != h)
                def _(h=h):
                    remote(
                        own_src, own_recv.at[z_hi], o_send, o_rsem, me, slab_of(x, h, 1)
                    ).start()

                @pl.when(z_hi == h)
                def _(h=h):
                    own_recv[h] = own_src[...]

        @pl.when(z_hi < heads)
        def _():
            with jax.named_scope("l_pairwait"):
                arrived(many(z_hi_n * pair_rows), p_rsem)
                if z_hi_n > 1:
                    arrived(own_recv.at[pl.ds(0, z_hi_n - 1)], o_rsem)

            with jax.named_scope("m_coh"):
                load_order.wait()
                own = ordered_sum([own_recv[h] for h in range(z_hi_n)])
                energy = own[snaps : 2 * snaps]
                for t in range(snaps):
                    spec_rows[t] = energy[t : t + 1]
                spec = spec_rows[me]
                final[snaps : snaps + 1, :] = spec

                def pair(i, d):
                    if i == 0:
                        return own[2 * d - 2 : 2 * d]
                    at = pairs_at[i].index(d)
                    return ordered_sum(
                        [pair_recv[h, steps.index(i), at] for h in range(z_hi_n)]
                    )

                def power(rows):
                    re, im = rows[0:1], rows[1:2]
                    return re * re + im * im

                def put_row(e, value):
                    coh_rows[e] = value / (spec * spec_rows[(me + snaps - e) % snaps])

                put_row(0, spec * spec)
                for d in range(1, half):
                    put_row(d, power(pair((d + 1) // 2, d)))
                    put_row(snaps - d, power(pair(-(d // 2), d)))
                re = pair((half + 1) // 2, half)[0:1]
                im = pair(-(half // 2), half)[0:1]
                put_row(half, re * re + im * im)
                for j in range(snaps):
                    final[j : j + 1, :] = coh_rows[(me - order_ref[j] + snaps) % snaps]
                forward_all()

        @pl.when(z_hi >= heads)
        def _():
            with jax.named_scope("n_finalwait"):
                arrived(final, f_rsem)
                load_order.wait()

    @pl.when(core == 0)
    def _():
        with jax.named_scope("n_finalwait"):
            arrived(final, f_rsem)

    with jax.named_scope("o_end"):
        out_ref[...] = final[0 : snaps + 1]
        @pl.when(core == 0)
        def _():
            left(src, m_send)
            left(peer_ids.at[0], i_send)
            left(spec_out, e_send)

        @pl.when(core == 1)
        def _():
            left(src.at[:, pl.ds(0, (snaps - 1) * ROWS)], m_send)
            left(r_recv.at[pl.ds(0, snaps - 1)], r_send)
            if x_n > 1:
                left(x_recv.at[pl.ds(0, x_n - 1)], x_send)
                left(spec_x.at[pl.ds(0, x_n - 1)], t_send)
            left(spec_recv.at[pl.ds(0, snaps - 1)], s_send)
            left(many(heads * pair_rows), p_send)

            @pl.when(z_hi < heads)
            def _():
                if heads > 1:
                    left(own_recv.at[pl.ds(0, heads - 1)], o_send)
                forwards_left()

            @pl.when(z_hi >= heads)
            def _():
                left(own_recv.at[pl.ds(0, heads)], o_send)


def finish(snaps, done_ref, coh_ref, spec_ref, sem):
    coh = pltpu.make_async_copy(done_ref.at[0:snaps], coh_ref.at[0], sem.at[0])
    spec = pltpu.make_async_copy(done_ref.at[snaps : snaps + 1], spec_ref, sem.at[1])
    coh.start()
    spec.start()
    coh.wait()
    spec.wait()


def body(sizes, velocity, shell_index, ref_order):
    snaps, x_n, z_hi_n = sizes
    half = snaps // 2
    heads = min(2, z_hi_n)
    lanes_n = velocity.shape[3] // LANES
    vel = velocity.reshape(3, 2, lanes_n, LANES).transpose(0, 2, 1, 3)
    vel = vel.reshape(3, 2 * lanes_n, LANES)
    ids = shell_index.reshape(lanes_n, LANES)
    f32, bf16, dma = jnp.float32, jnp.bfloat16, pltpu.SemaphoreType.DMA
    done = pl.pallas_call(
        functools.partial(kernel, sizes),
        out_shape=pltpu.VMEM((snaps + 1, SHELLS), f32),
        in_specs=[pl.BlockSpec(memory_space=pl.ANY)] * 3,
        out_specs=pl.BlockSpec(memory_space=pltpu.VMEM),
        scratch_shapes=[
            pltpu.VMEM((3, 2 * lanes_n, LANES), bf16),
            pltpu.VMEM((SETS, HALVES, snaps, 3, PIECE, LANES), bf16),
            pltpu.VMEM((lanes_n, LANES), jnp.int32),
            pltpu.VMEM((2, GROUPS, LANES), jnp.int32),
            pltpu.SMEM((snaps,), jnp.int32),
            pltpu.VMEM((3, (snaps + half + 1) * PITCH, LANES), f32),
            pltpu.VMEM(((snaps - 1) * snaps, GROUPS * LANES), bf16),
            pltpu.VMEM((SETS, SHELLS, GROUPS * LANES), bf16),
            pltpu.VMEM(((snaps - 1) * snaps, SHELLS), f32),
            pltpu.VMEM((snaps * snaps, SHELLS), f32),
            pltpu.VMEM((snaps, snaps, SHELLS), f32),
            pltpu.VMEM((x_n, snaps, SHELLS), f32),
            pltpu.VMEM((1, SHELLS), f32),
            pltpu.VMEM((1, SHELLS), f32),
            pltpu.VMEM((x_n, 1, SHELLS), f32),
            pltpu.VMEM((snaps, 1, SHELLS), f32),
            pltpu.VMEM((2 * snaps, SHELLS), f32),
            pltpu.VMEM((z_hi_n, 2 * snaps, SHELLS), f32),
            pltpu.VMEM((half, 2, SHELLS), f32),
            pltpu.VMEM((z_hi_n, half, 2, 2, SHELLS), f32),
            pltpu.VMEM((snaps, 1, SHELLS), f32),
            pltpu.VMEM((snaps, 1, SHELLS), f32),
            pltpu.VMEM((OUT_ROWS, SHELLS), f32),
            dma((3,)),
            dma(()),
            dma((SETS, HALVES)),
            dma(()),
            dma((2,)),
            *[dma(())] * 16,
        ],
        compiler_params=pltpu.CompilerParams(collective_id=0, has_side_effects=True),
    )(vel, ids, ref_order)
    return pl.pallas_call(
        functools.partial(finish, snaps),
        out_shape=(
            jax.ShapeDtypeStruct((1, snaps, SHELLS), f32),
            jax.ShapeDtypeStruct((1, SHELLS), f32),
        ),
        in_specs=[pl.BlockSpec(memory_space=pltpu.VMEM)],
        out_specs=(pl.BlockSpec(memory_space=pl.ANY),) * 2,
        scratch_shapes=[dma((2,))],
    )(pltpu.with_memory_space_constraint(done, pltpu.VMEM))


def solution(mesh):
    snaps, slabs = mesh.shape["tm"], mesh.shape["slab"]
    z_hi_n = min(Z_HI, slabs // CORES)
    sizes = (snaps, slabs // CORES // z_hi_n, z_hi_n)
    return jax.shard_map(
        functools.partial(body, sizes),
        mesh=mesh,
        in_specs=(P("tm", None, None, "slab"), P("slab"), P()),
        out_specs=(P("tm", None, None), P("tm", None)),
        check_vma=False,
    )
```

```python
import functools

import jax
import jax.numpy as jnp
from jax import lax
from jax.experimental import pallas as pl
from jax.experimental.pallas import tpu as pltpu
from jax.sharding import PartitionSpec as P

SHELLS = 128
LANES = 128
Z_LO, Z_HI, CORES = 2, 4, 2
ROWS = 16
GROUPS = ROWS // 2
PITCH = ROWS + 1
SETS = 3
HALVES = 2
PIECE = ROWS // HALVES
OUT_ROWS = 24


def remote(src, dst, send_sem, recv_sem, tm, slab):
    return pltpu.make_async_remote_copy(
        src_ref=src,
        dst_ref=dst,
        send_sem=send_sem,
        recv_sem=recv_sem,
        device_id={"tm": tm, "slab": slab},
        device_id_type=pl.DeviceIdType.MESH,
    )


def arrived(ref, sem):
    remote(ref, ref, sem, sem, lax.axis_index("tm"), lax.axis_index("slab")).wait_recv()


def left(ref, sem):
    remote(ref, ref, sem, sem, lax.axis_index("tm"), lax.axis_index("slab")).wait_send()


def ordered_sum(terms):
    total = terms[0]
    for term in terms[1:]:
        total = total + term
    return total


def kernel(
    sizes,
    vel_ref,
    shell_ref,
    order_hbm,
    out_ref,
    src,
    recv,
    all_ids,
    peer_ids,
    order_ref,
    wide,
    terms,
    onehot,
    binned,
    sums,
    r_recv,
    x_recv,
    spec_out,
    spec_peer,
    spec_x,
    spec_recv,
    own_src,
    own_recv,
    pair_src,
    pair_recv,
    spec_rows,
    coh_rows,
    final,
    load_sem,
    m_send,
    m_recv,
    i_send,
    i_recv,
    r_send,
    r_rsem,
    x_send,
    x_rsem,
    p_send,
    p_rsem,
    h_send,
    h_rsem,
    o_send,
    o_rsem,
    e_send,
    e_rsem,
    s_send,
    s_rsem,
    t_send,
    t_rsem,
    f_send,
    f_rsem,
):
    snaps, x_n, z_hi_n = sizes
    half = snaps // 2
    heads = min(2, z_hi_n)
    me = lax.axis_index("tm")
    slab = lax.axis_index("slab")
    core = slab % CORES
    x, z_hi = slab // CORES // z_hi_n, slab // CORES % z_hi_n
    y_n, z_n = snaps // Z_LO, z_hi_n * Z_LO
    y, z_lo = me // Z_LO, me % Z_LO
    z = z_hi * Z_LO + z_lo
    base = y * Z_LO
    block = Z_LO * snaps
    far = slab - core
    near = far + 1
    late = z_hi_n - 1 - z_hi
    is_late = z_hi // heads
    part_set = core + (1 - core) * 2 * is_late
    by_distance = sorted(range(1, snaps), key=lambda d: (-min(d, snaps - d), d))

    pairs_at = {0: (1,)}
    for step in range(1, (half + 1) // 2 + 1):
        pairs_at[step] = tuple(d for d in (2 * step - 1, 2 * step) if d <= half)
    for step in range(1, half // 2 + 1):
        pairs_at[-step] = tuple(d for d in (2 * step, 2 * step + 1) if d <= half)
    y_steps = sorted(range(1, y_n), key=lambda d: -min(d, y_n - d))
    x_steps = sorted(range(1, x_n), key=lambda d: -min(d, x_n - d))
    messages = sorted(
        ((k, i) for k in range(Z_LO) for i in pairs_at), key=lambda m: (-abs(m[1]), m)
    )
    away = [(k, i) for k, i in messages if not 0 <= k + i < Z_LO]
    at_home = [(k, i) for k, i in messages if 0 <= k + i < Z_LO]
    away_rows = sum(2 * len(pairs_at[i]) for _, i in away)
    reach = sorted({k + i for k, i in messages})
    slots = list(pairs_at)

    def there(d):
        return (me + d) % snaps

    def whence(d):
        return (me + snaps - d) % snaps

    def slab_of(xx, zz, cc):
        return (xx * z_hi_n + zz) * CORES + cc

    def many(n):
        if n <= r_recv.shape[1]:
            return r_recv.at[0, pl.ds(0, n)]
        if 2 * n > vel_ref.shape[1]:
            return vel_ref.at[pl.ds(0, 2), pl.ds(0, n)]
        return vel_ref.at[0, pl.ds(0, 2 * n)]

    def home_rows(n):
        return pair_recv.at[pl.ds(0, n), pl.ds(0, 3), 0]

    def rows_of(t, n):
        return pl.ds(pl.multiple_of(t * n, n), n)

    load_all = pltpu.make_async_copy(vel_ref, src, load_sem.at[0])
    load_all.start()
    load_ids = pltpu.make_async_copy(shell_ref, all_ids, load_sem.at[1])
    load_ids.start()
    load_own = [
        pltpu.make_async_copy(
            vel_ref.at[:, pl.ds(pl.multiple_of(me * ROWS + n * PIECE, PIECE), PIECE)],
            recv.at[1, n, me],
            m_recv.at[1, n],
        )
        for n in range(HALVES)
    ]
    load_order = pltpu.make_async_copy(order_hbm, order_ref, load_sem.at[2])

    barrier = pltpu.get_barrier_semaphore()

    def greet(tm, sl):
        pl.semaphore_signal(
            barrier, inc=1, device_id={"tm": tm, "slab": sl}, device_id_type=pl.DeviceIdType.MESH
        )

    with jax.named_scope("a_greet"):

        @pl.when(core == 1)
        def _():
            @pl.when(z_hi < heads)
            def _():
                @pl.when(late >= heads)
                def _():
                    for d in [*by_distance, 0]:
                        greet(there(d), slab_of(x, late, 0))

                for d in by_distance:
                    greet(there(d), near)
                    greet(there(d), far)

            @pl.when(z_hi >= heads)
            def _():
                for d in by_distance:
                    greet(there(d), near)

            greet(me, far)
            for d in range(1, x_n):
                greet(there(0), slab_of((x + d) % x_n, z_hi, 1))

        @pl.when(core == 1)
        def _():
            for copy in load_own:
                copy.start()
            load_order.start()

            @pl.when(z_hi < heads)
            def _():
                for h in range(1, z_hi_n):
                    for i in reach:
                        greet((base + snaps + i) % snaps, slab_of(x, (z_hi + h) % z_hi_n, 1))

    with jax.named_scope("b_barrier"):

        @pl.when(core == 0)
        def _():
            @pl.when(z_hi < heads)
            def _():
                pl.semaphore_wait(barrier, snaps)

            @pl.when(z_hi >= heads)
            def _():
                pl.semaphore_wait(barrier, snaps + 1)

        @pl.when(core == 1)
        def _():
            @pl.when(z_hi < heads)
            def _():
                pl.semaphore_wait(barrier, snaps - 1 + x_n - 1 + (heads - 1) * len(reach))

            @pl.when(z_hi >= heads)
            def _():
                pl.semaphore_wait(barrier, snaps - 1 + x_n - 1 + heads * len(reach))

    def part_copy(n, d):
        return remote(
            src.at[:, pl.ds(pl.multiple_of(there(d) * ROWS + n * PIECE, PIECE), PIECE)],
            recv.at[part_set, n, me],
            m_send,
            m_recv.at[part_set, n],
            there(d),
            slab_of(x, z_hi + (1 - core) * is_late * (late - z_hi), 1),
        )

    def ids_copy():
        return remote(
            all_ids.at[rows_of(me, GROUPS)],
            peer_ids.at[is_late],
            i_send,
            i_recv.at[is_late],
            me,
            slab_of(x, z_hi + is_late * (late - z_hi), 1),
        )

    def spec_copy():
        return remote(spec_out, spec_peer, e_send, e_rsem, me, near)

    shells = lax.broadcasted_iota(jnp.int32, (SHELLS, LANES), 0)

    def local_spectrum():
        lanes_n = shell_ref.shape[0]
        squares = ordered_sum([src[c].astype(jnp.float32) ** 2 for c in range(3)])
        wide[0, 0 : 2 * lanes_n, :] = squares
        energy = wide[0, pl.ds(0, lanes_n, stride=2), :] + wide[0, pl.ds(1, lanes_n, stride=2), :]
        wide[1, 0:lanes_n, :] = energy.astype(jnp.bfloat16).astype(jnp.float32)

        def add_rows(i, total):
            at = rows_of(i, 8)
            shell, value = all_ids[at, :], wide[1, at, :]
            for r in range(8):
                hit = jnp.broadcast_to(shell[r : r + 1], (SHELLS, LANES)) == shells
                total = total + jnp.where(
                    hit, jnp.broadcast_to(value[r : r + 1], (SHELLS, LANES)), 0.0
                )
            return total

        by_lane = lax.fori_loop(
            0, lanes_n // 8, add_rows, jnp.zeros((SHELLS, LANES), jnp.float32)
        )
        return lax.dot_general(
            jnp.ones((8, LANES), jnp.float32),
            by_lane,
            (((1,), (1,)), ((), ())),
            precision=lax.Precision.HIGHEST,
            preferred_element_type=jnp.float32,
        )[0:1]

    ahead = 1 if x_n > 1 else 0
    first_head = (me == 0) & (z_hi == 0)

    def forward(xx, zz, c):
        remote(final, final, f_send, f_rsem, me, slab_of(xx, zz, c)).start()

    def forward_all():
        for xx in range(x_n):

            @pl.when(x == xx)
            def _(xx=xx):
                if xx or not ahead:
                    forward(xx, z_hi, 0)
                else:

                    @pl.when(jnp.logical_not(first_head))
                    def _():
                        forward(xx, z_hi, 0)

                if xx == ahead and xx:

                    @pl.when(first_head)
                    def _():
                        forward(0, z_hi, 0)

                @pl.when(late >= heads)
                def _():
                    for to in {0: () if ahead else (0,), 1: (0, 1)}.get(xx, (xx,)):
                        forward(to, late, 1)
                        forward(to, late, 0)

    def forwards_left():
        for xx in range(x_n):
            for is_first in (False, True):
                for has_late in (False, True):
                    copies = 1
                    if xx == 0 and ahead and is_first:
                        copies -= 1
                    if xx == 1 and is_first:
                        copies += 1
                    if has_late:
                        copies += 2 * len({0: () if ahead else (0,), 1: (0, 1)}.get(xx, (xx,)))
                    if copies:

                        @pl.when(
                            (x == xx)
                            & (first_head == is_first)
                            & ((late >= heads) == has_late)
                        )
                        def _(copies=copies):
                            left(many(copies * OUT_ROWS), f_send)

    load_all.wait()

    @pl.when(core == 0)
    def _():
        for n in range(HALVES):
            for d in [*by_distance, 0]:
                part_copy(n, d).start()
        load_ids.wait()
        ids_copy().start()
        spec_out[...] = local_spectrum()
        spec_copy().start()

    @pl.when(core == 1)
    def _():
        for n in range(HALVES):
            for d in by_distance:
                part_copy(n, d).start()

        first = lax.broadcasted_iota(jnp.int32, (snaps, LANES), 0) < half

        def spread_shells(c):
            for g in range(GROUPS):
                if c == 1:
                    row = all_ids[pl.ds(me * GROUPS + g, 1), :]
                else:
                    row = peer_ids[c // 2, g : g + 1, :]
                row = jnp.broadcast_to(row, (SHELLS, LANES))
                hot = jnp.where(row == shells, 1.0, 0.0).astype(jnp.bfloat16)
                onehot[c, :, g * LANES : (g + 1) * LANES] = hot

        def widen(core_of, n):
            for t in range(snaps):
                for c in range(3):
                    value = recv[core_of, n, t, c].astype(jnp.float32)
                    for at in (t, t + snaps) if t < half else (t,):
                        row = at * PITCH + n * PIECE
                        wide[c, row : row + PIECE, :] = value

        def products(g):
            def rows(c, p, d):
                return wide[c, pl.ds(d * PITCH + 2 * g + p, snaps, stride=PITCH), :]

            def put(k, value):
                terms[k * snaps : (k + 1) * snaps, g * LANES : (g + 1) * LANES] = value.astype(
                    jnp.bfloat16
                )

            own = [[rows(c, p, 0) for p in range(2)] for c in range(3)]
            for d in range(1, half + 1):
                other = [[rows(c, p, d) for p in range(2)] for c in range(3)]
                real = sum(own[c][p] * other[c][p] for c in range(3) for p in range(2))
                imag = sum(own[c][1] * other[c][0] - own[c][0] * other[c][1] for c in range(3))
                if d < half:
                    put(2 * d - 2, real)
                    put(2 * d - 1, imag)
                else:
                    put(2 * d - 2, jnp.where(first, real, imag))

        def bin_part(core_of, q):
            for g in (2 * q, 2 * q + 1):
                products(g)
            modes = slice(2 * q * LANES, 2 * (q + 1) * LANES)
            return lax.dot_general(
                terms[:, modes],
                onehot[core_of, :, modes],
                (((1,), (1,)), ((), ())),
                preferred_element_type=jnp.float32,
            )

        with jax.named_scope("c_onehot"):
            load_ids.wait()
            spread_shells(1)

            @pl.when(z_hi < heads)
            def _():
                arrived(peer_ids.at[0], i_recv.at[0])
                spread_shells(0)

        with jax.named_scope("c_spectrum"):
            mine = local_spectrum()
            spec_copy().wait_recv()
            spec_x[x] = mine + spec_peer[...]
            for d in x_steps:
                remote(
                    spec_x.at[x],
                    spec_x.at[x],
                    t_send,
                    t_rsem,
                    me,
                    slab_of((x + d) % x_n, z_hi, 1),
                ).start()

        quarters = GROUPS // 2 // HALVES

        def work_off(c, n):
            with jax.named_scope(f"d_wait{c}{n}"):
                arrived(recv.at[c, n], m_recv.at[c, n])
            with jax.named_scope(f"e_work{c}{n}"):
                widen(c, n)
                for q in range(n * quarters, (n + 1) * quarters):
                    if (c, q) == (1, 0):
                        binned[...] = bin_part(c, q)
                    else:
                        binned[...] += bin_part(c, q)

        for n in range(HALVES):
            work_off(1, n)

            @pl.when(z_hi < heads)
            def _(n=n):
                work_off(0, n)

        @pl.when((z_hi < heads) & (late >= heads))
        def _():
            arrived(peer_ids.at[1], i_recv.at[1])
            spread_shells(2)
            for n in range(HALVES):
                work_off(2, n)

        with jax.named_scope("g_turn"):
            for k in range(snaps - 1):
                value, shift = binned[k * snaps : (k + 1) * snaps], (k // 2 + 1) // 2
                sums[pl.ds(shift * snaps + k, snaps - shift, stride=snaps), :] = value[
                    0 : snaps - shift
                ]
                if shift:
                    sums[pl.ds(k, shift, stride=snaps), :] = value[snaps - shift :]
            sums[pl.ds(snaps - 1, snaps, stride=snaps), :] = jnp.zeros((snaps, SHELLS), jnp.float32)

        with jax.named_scope("h_owner"):
            for d in y_steps:
                yy = (y + d) % y_n
                remote(
                    sums.at[rows_of(yy, block)],
                    r_recv.at[y],
                    r_send,
                    r_rsem,
                    yy * Z_LO + z_lo,
                    slab,
                ).start()
            r_recv[y] = sums[rows_of(y, block), :]
            if x_n > 1:
                arrived(spec_x.at[pl.ds(0, x_n - 1)], t_rsem)
            spec_recv[me] = ordered_sum([spec_x[i] for i in range(x_n)])
            for d in by_distance:
                remote(
                    spec_recv.at[me], spec_recv.at[me], s_send, s_rsem, there(d), slab
                ).start()
            arrived(r_recv.at[pl.ds(0, y_n - 1)], r_rsem)
            x_recv[x] = ordered_sum([r_recv[i] for i in range(y_n)])

        with jax.named_scope("i_x"):
            for d in x_steps:
                remote(
                    x_recv.at[x],
                    x_recv.at[x],
                    x_send,
                    x_rsem,
                    me,
                    slab_of((x + d) % x_n, z_hi, 1),
                ).start()
            if x_n > 1:
                arrived(x_recv.at[pl.ds(0, x_n - 1)], x_rsem)
            total = ordered_sum([x_recv[i] for i in range(x_n)])
            arrived(spec_recv.at[pl.ds(0, snaps - 1)], s_rsem)

        with jax.named_scope("j_pairs"):
            for t in range(snaps):
                own_src[t : t + 1, :] = spec_recv[t]
            for k in range(Z_LO):
                for d in range(1, half + 1):
                    row = k * snaps + 2 * d - 2
                    pair_src[k, d - 1] = total[row : row + 2]

        def pair_copy(h, k, i, send_sem, recv_sem):
            count = len(pairs_at[i])
            return remote(
                pair_src.at[k, pl.ds(pairs_at[i][0] - 1, count)],
                pair_recv.at[z, slots.index(i), pl.ds(0, count)],
                send_sem,
                recv_sem,
                (base + snaps + k + i) % snaps,
                slab_of(x, h, 1),
            )

        with jax.named_scope("k_send"):
            for h in range(heads):
                for k, i in away:
                    pair_copy(h, k, i, p_send, p_rsem).start()
                for k, i in at_home:
                    here = (z_hi == h) & (z_lo == k + i)

                    @pl.when(here)
                    def _(k=k, i=i):
                        first_pair, count = pairs_at[i][0] - 1, len(pairs_at[i])
                        pair_recv[z, slots.index(i), 0:count] = pair_src[
                            k, first_pair : first_pair + count
                        ]

                    @pl.when(jnp.logical_not(here))
                    def _(h=h, k=k, i=i):
                        pair_copy(h, k, i, h_send, h_rsem).start()

                @pl.when(z_hi != h)
                def _(h=h):
                    remote(
                        own_src, own_recv.at[z_hi], o_send, o_rsem, me, slab_of(x, h, 1)
                    ).start()

                @pl.when(z_hi == h)
                def _(h=h):
                    own_recv[h] = own_src[...]

        @pl.when(z_hi < heads)
        def _():
            with jax.named_scope("l_pairwait"):
                arrived(many(z_n * away_rows // Z_LO), p_rsem)
                arrived(home_rows(z_n - 1), h_rsem)
                if z_hi_n > 1:
                    arrived(own_recv.at[pl.ds(0, z_hi_n - 1)], o_rsem)

            with jax.named_scope("m_coh"):
                load_order.wait()
                own = ordered_sum([own_recv[h] for h in range(z_hi_n)])
                for t in range(snaps):
                    spec_rows[t] = own[t : t + 1]
                spec = spec_rows[me]
                final[snaps : snaps + 1, :] = spec

                def pair(i, d):
                    at = pairs_at[i].index(d)
                    return ordered_sum([pair_recv[p, slots.index(i), at] for p in range(z_n)])

                def power(rows):
                    re, im = rows[0:1], rows[1:2]
                    return re * re + im * im

                def put_row(e, value):
                    coh_rows[e] = value / (spec * spec_rows[(me + snaps - e) % snaps])

                put_row(0, spec * spec)
                for d in range(1, half):
                    put_row(d, power(pair((d + 1) // 2, d)))
                    put_row(snaps - d, power(pair(-(d // 2), d)))
                re = pair((half + 1) // 2, half)[0:1]
                im = pair(-(half // 2), half)[0:1]
                put_row(half, re * re + im * im)
                for j in range(snaps):
                    final[j : j + 1, :] = coh_rows[(me - order_ref[j] + snaps) % snaps]
                forward_all()

        @pl.when(z_hi >= heads)
        def _():
            with jax.named_scope("n_finalwait"):
                arrived(final, f_rsem)
                load_order.wait()

    @pl.when(core == 0)
    def _():
        with jax.named_scope("n_finalwait"):
            arrived(final, f_rsem)

    with jax.named_scope("o_end"):
        out_ref[...] = final[0 : snaps + 1]
        @pl.when(core == 0)
        def _():
            left(src, m_send)
            left(peer_ids.at[0], i_send)
            left(spec_out, e_send)

        @pl.when(core == 1)
        def _():
            left(src.at[:, pl.ds(0, (snaps - 1) * ROWS)], m_send)
            left(r_recv.at[pl.ds(0, y_n - 1)], r_send)
            if x_n > 1:
                left(x_recv.at[pl.ds(0, x_n - 1)], x_send)
                left(spec_x.at[pl.ds(0, x_n - 1)], t_send)
            left(spec_recv.at[pl.ds(0, snaps - 1)], s_send)
            left(many(heads * away_rows), p_send)

            @pl.when(z_hi < heads)
            def _():
                left(home_rows(heads * Z_LO - 1), h_send)
                if heads > 1:
                    left(own_recv.at[pl.ds(0, heads - 1)], o_send)
                forwards_left()

            @pl.when(z_hi >= heads)
            def _():
                left(home_rows(heads * Z_LO), h_send)
                left(own_recv.at[pl.ds(0, heads)], o_send)


def finish(snaps, done_ref, coh_ref, spec_ref, sem):
    coh = pltpu.make_async_copy(done_ref.at[0:snaps], coh_ref.at[0], sem.at[0])
    spec = pltpu.make_async_copy(done_ref.at[snaps : snaps + 1], spec_ref, sem.at[1])
    coh.start()
    spec.start()
    coh.wait()
    spec.wait()


def body(sizes, velocity, shell_index, ref_order):
    snaps, x_n, z_hi_n = sizes
    half = snaps // 2
    heads = min(2, z_hi_n)
    lanes_n = velocity.shape[3] // LANES
    vel = velocity.reshape(3, 2, lanes_n, LANES).transpose(0, 2, 1, 3)
    vel = vel.reshape(3, 2 * lanes_n, LANES)
    ids = shell_index.reshape(lanes_n, LANES)
    f32, bf16, dma = jnp.float32, jnp.bfloat16, pltpu.SemaphoreType.DMA
    done = pl.pallas_call(
        functools.partial(kernel, sizes),
        out_shape=pltpu.VMEM((snaps + 1, SHELLS), f32),
        in_specs=[pl.BlockSpec(memory_space=pl.ANY)] * 3,
        out_specs=pl.BlockSpec(memory_space=pltpu.VMEM),
        scratch_shapes=[
            pltpu.VMEM((3, 2 * lanes_n, LANES), bf16),
            pltpu.VMEM((SETS, HALVES, snaps, 3, PIECE, LANES), bf16),
            pltpu.VMEM((lanes_n, LANES), jnp.int32),
            pltpu.VMEM((2, GROUPS, LANES), jnp.int32),
            pltpu.SMEM((snaps,), jnp.int32),
            pltpu.VMEM((3, (snaps + half + 1) * PITCH, LANES), f32),
            pltpu.VMEM(((snaps - 1) * snaps, GROUPS * LANES), bf16),
            pltpu.VMEM((SETS, SHELLS, GROUPS * LANES), bf16),
            pltpu.VMEM(((snaps - 1) * snaps, SHELLS), f32),
            pltpu.VMEM((snaps * snaps, SHELLS), f32),
            pltpu.VMEM((snaps // Z_LO, Z_LO * snaps, SHELLS), f32),
            pltpu.VMEM((x_n, Z_LO * snaps, SHELLS), f32),
            pltpu.VMEM((1, SHELLS), f32),
            pltpu.VMEM((1, SHELLS), f32),
            pltpu.VMEM((x_n, 1, SHELLS), f32),
            pltpu.VMEM((snaps, 1, SHELLS), f32),
            pltpu.VMEM((snaps, SHELLS), f32),
            pltpu.VMEM((z_hi_n, snaps, SHELLS), f32),
            pltpu.VMEM((Z_LO, half, 2, SHELLS), f32),
            pltpu.VMEM((z_hi_n * Z_LO, half + 1, 2, 2, SHELLS), f32),
            pltpu.VMEM((snaps, 1, SHELLS), f32),
            pltpu.VMEM((snaps, 1, SHELLS), f32),
            pltpu.VMEM((OUT_ROWS, SHELLS), f32),
            dma((3,)),
            dma(()),
            dma((SETS, HALVES)),
            dma(()),
            dma((2,)),
            *[dma(())] * 18,
        ],
        compiler_params=pltpu.CompilerParams(collective_id=0, has_side_effects=True),
    )(vel, ids, ref_order)
    return pl.pallas_call(
        functools.partial(finish, snaps),
        out_shape=(
            jax.ShapeDtypeStruct((1, snaps, SHELLS), f32),
            jax.ShapeDtypeStruct((1, SHELLS), f32),
        ),
        in_specs=[pl.BlockSpec(memory_space=pltpu.VMEM)],
        out_specs=(pl.BlockSpec(memory_space=pl.ANY),) * 2,
        scratch_shapes=[dma((2,))],
    )(pltpu.with_memory_space_constraint(done, pltpu.VMEM))


def solution(mesh):
    snaps, slabs = mesh.shape["tm"], mesh.shape["slab"]
    z_hi_n = min(Z_HI, slabs // CORES)
    sizes = (snaps, slabs // CORES // z_hi_n, z_hi_n)
    return jax.shard_map(
        functools.partial(body, sizes),
        mesh=mesh,
        in_specs=(P("tm", None, None, "slab"), P("slab"), P()),
        out_specs=(P("tm", None, None), P("tm", None)),
        check_vma=False,
    )
```

```python
import functools

import jax
import jax.numpy as jnp
from jax import lax
from jax.experimental import pallas as pl
from jax.experimental.pallas import tpu as pltpu
from jax.sharding import PartitionSpec as P

SHELLS = 128
LANES = 128
Z_LO, Z_HI, CORES = 2, 4, 2
ROWS = 16
GROUPS = ROWS // 2
PITCH = ROWS + 1
SETS = 3
HALVES = 2
PIECE = ROWS // HALVES
OUT_ROWS = 24


def remote(src, dst, send_sem, recv_sem, tm, slab):
    return pltpu.make_async_remote_copy(
        src_ref=src,
        dst_ref=dst,
        send_sem=send_sem,
        recv_sem=recv_sem,
        device_id={"tm": tm, "slab": slab},
        device_id_type=pl.DeviceIdType.MESH,
    )


def arrived(ref, sem):
    remote(ref, ref, sem, sem, lax.axis_index("tm"), lax.axis_index("slab")).wait_recv()


def left(ref, sem):
    remote(ref, ref, sem, sem, lax.axis_index("tm"), lax.axis_index("slab")).wait_send()


def ordered_sum(terms):
    total = terms[0]
    for term in terms[1:]:
        total = total + term
    return total


def kernel(
    sizes,
    vel_ref,
    shell_ref,
    order_hbm,
    out_ref,
    src,
    recv,
    all_ids,
    peer_ids,
    order_ref,
    wide,
    terms,
    onehot,
    binned,
    sums,
    r_recv,
    x_recv,
    spec_out,
    spec_peer,
    spec_x,
    spec_recv,
    own_src,
    own_recv,
    pair_src,
    pair_recv,
    spec_rows,
    coh_rows,
    final,
    load_sem,
    m_send,
    m_recv,
    i_send,
    i_recv,
    r_send,
    r_rsem,
    x_send,
    x_rsem,
    p_send,
    p_rsem,
    h_send,
    h_rsem,
    o_send,
    o_rsem,
    e_send,
    e_rsem,
    s_send,
    s_rsem,
    t_send,
    t_rsem,
    f_send,
    f_rsem,
):
    snaps, x_n, z_hi_n = sizes
    half = snaps // 2
    heads = min(2, z_hi_n)
    me = lax.axis_index("tm")
    slab = lax.axis_index("slab")
    core = slab % CORES
    x, z_hi = slab // CORES // z_hi_n, slab // CORES % z_hi_n
    y_n, z_n = snaps // Z_LO, z_hi_n * Z_LO
    y, z_lo = me // Z_LO, me % Z_LO
    z = z_hi * Z_LO + z_lo
    base = y * Z_LO
    block = Z_LO * snaps
    far = slab - core
    near = far + 1
    late = z_hi_n - 1 - z_hi
    is_late = z_hi // heads
    part_set = core + (1 - core) * 2 * is_late
    by_distance = sorted(range(1, snaps), key=lambda d: (-min(d, snaps - d), d))
    far_ones, near_ones = by_distance[: half - 1], by_distance[half - 1 :]

    pairs_at = {0: (1,)}
    for step in range(1, (half + 1) // 2 + 1):
        pairs_at[step] = tuple(d for d in (2 * step - 1, 2 * step) if d <= half)
    for step in range(1, half // 2 + 1):
        pairs_at[-step] = tuple(d for d in (2 * step, 2 * step + 1) if d <= half)
    y_steps = sorted(range(1, y_n), key=lambda d: -min(d, y_n - d))
    x_steps = sorted(range(1, x_n), key=lambda d: -min(d, x_n - d))
    messages = sorted(
        ((k, i) for k in range(Z_LO) for i in pairs_at), key=lambda m: (-abs(m[1]), m)
    )
    away = [(k, i) for k, i in messages if not 0 <= k + i < Z_LO]
    at_home = [(k, i) for k, i in messages if 0 <= k + i < Z_LO]
    away_rows = sum(2 * len(pairs_at[i]) for _, i in away)
    reach = sorted({k + i for k, i in messages})
    slots = list(pairs_at)

    def there(d):
        return (me + d) % snaps

    def whence(d):
        return (me + snaps - d) % snaps

    def slab_of(xx, zz, cc):
        return (xx * z_hi_n + zz) * CORES + cc

    def many(n):
        if n <= r_recv.shape[1]:
            return r_recv.at[0, pl.ds(0, n)]
        if 2 * n > vel_ref.shape[1]:
            return vel_ref.at[pl.ds(0, 2), pl.ds(0, n)]
        return vel_ref.at[0, pl.ds(0, 2 * n)]

    def home_rows(n):
        return pair_recv.at[pl.ds(0, n), pl.ds(0, 3), 0]

    def rows_of(t, n):
        return pl.ds(pl.multiple_of(t * n, n), n)

    load_all = pltpu.make_async_copy(vel_ref, src, load_sem.at[0])
    load_all.start()
    load_ids = pltpu.make_async_copy(shell_ref, all_ids, load_sem.at[1])
    load_ids.start()
    load_own = [
        pltpu.make_async_copy(
            vel_ref.at[:, pl.ds(pl.multiple_of(me * ROWS + n * PIECE, PIECE), PIECE)],
            recv.at[1, n, me],
            m_recv.at[1, n],
        )
        for n in range(HALVES)
    ]
    load_order = pltpu.make_async_copy(order_hbm, order_ref, load_sem.at[2])

    barrier = pltpu.get_barrier_semaphore()

    def greet(tm, sl):
        pl.semaphore_signal(
            barrier, inc=1, device_id={"tm": tm, "slab": sl}, device_id_type=pl.DeviceIdType.MESH
        )

    with jax.named_scope("a_greet"):

        @pl.when(core == 1)
        def _():
            @pl.when(z_hi < heads)
            def _():
                @pl.when(late >= heads)
                def _():
                    for d in [*by_distance, 0]:
                        greet(there(d), slab_of(x, late, 0))

                for d in by_distance:
                    greet(there(d), near)
                    greet(there(d), far)

            @pl.when(z_hi >= heads)
            def _():
                for d in by_distance:
                    greet(there(d), near)

            greet(me, far)
            for d in range(1, x_n):
                greet(there(0), slab_of((x + d) % x_n, z_hi, 1))

        @pl.when(core == 1)
        def _():
            for copy in load_own:
                copy.start()
            load_order.start()

            @pl.when(z_hi < heads)
            def _():
                for h in range(1, z_hi_n):
                    for i in reach:
                        greet((base + snaps + i) % snaps, slab_of(x, (z_hi + h) % z_hi_n, 1))

    with jax.named_scope("b_barrier"):

        @pl.when(core == 0)
        def _():
            @pl.when(z_hi < heads)
            def _():
                pl.semaphore_wait(barrier, snaps)

            @pl.when(z_hi >= heads)
            def _():
                pl.semaphore_wait(barrier, snaps + 1)

        @pl.when(core == 1)
        def _():
            @pl.when(z_hi < heads)
            def _():
                pl.semaphore_wait(barrier, snaps - 1 + x_n - 1 + (heads - 1) * len(reach))

            @pl.when(z_hi >= heads)
            def _():
                pl.semaphore_wait(barrier, snaps - 1 + x_n - 1 + heads * len(reach))

    def part_copy(n, d):
        return remote(
            src.at[:, pl.ds(pl.multiple_of(there(d) * ROWS + n * PIECE, PIECE), PIECE)],
            recv.at[part_set, n, me],
            m_send,
            m_recv.at[part_set, n],
            there(d),
            slab_of(x, z_hi + (1 - core) * is_late * (late - z_hi), 1),
        )

    def ids_copy():
        return remote(
            all_ids.at[rows_of(me, GROUPS)],
            peer_ids.at[is_late],
            i_send,
            i_recv.at[is_late],
            me,
            slab_of(x, z_hi + is_late * (late - z_hi), 1),
        )

    def spec_copy():
        return remote(spec_out, spec_peer, e_send, e_rsem, me, near)

    shells = lax.broadcasted_iota(jnp.int32, (SHELLS, LANES), 0)

    def local_spectrum():
        lanes_n = shell_ref.shape[0]
        squares = ordered_sum([src[c].astype(jnp.float32) ** 2 for c in range(3)])
        wide[0, 0 : 2 * lanes_n, :] = squares
        energy = wide[0, pl.ds(0, lanes_n, stride=2), :] + wide[0, pl.ds(1, lanes_n, stride=2), :]
        wide[1, 0:lanes_n, :] = energy.astype(jnp.bfloat16).astype(jnp.float32)

        def add_rows(i, total):
            at = rows_of(i, 8)
            shell, value = all_ids[at, :], wide[1, at, :]
            for r in range(8):
                hit = jnp.broadcast_to(shell[r : r + 1], (SHELLS, LANES)) == shells
                total = total + jnp.where(
                    hit, jnp.broadcast_to(value[r : r + 1], (SHELLS, LANES)), 0.0
                )
            return total

        by_lane = lax.fori_loop(
            0, lanes_n // 8, add_rows, jnp.zeros((SHELLS, LANES), jnp.float32)
        )
        return lax.dot_general(
            jnp.ones((8, LANES), jnp.float32),
            by_lane,
            (((1,), (1,)), ((), ())),
            precision=lax.Precision.HIGHEST,
            preferred_element_type=jnp.float32,
        )[0:1]

    ahead = 1 if x_n > 1 else 0
    first_head = (me == 0) & (z_hi == 0)

    def forward(xx, zz, c):
        remote(final, final, f_send, f_rsem, me, slab_of(xx, zz, c)).start()

    def forward_all():
        for xx in range(x_n):

            @pl.when(x == xx)
            def _(xx=xx):
                if xx or not ahead:
                    forward(xx, z_hi, 0)
                else:

                    @pl.when(jnp.logical_not(first_head))
                    def _():
                        forward(xx, z_hi, 0)

                if xx == ahead and xx:

                    @pl.when(first_head)
                    def _():
                        forward(0, z_hi, 0)

                @pl.when(late >= heads)
                def _():
                    for to in {0: () if ahead else (0,), 1: (0, 1)}.get(xx, (xx,)):
                        forward(to, late, 1)
                        forward(to, late, 0)

    def forwards_left():
        for xx in range(x_n):
            for is_first in (False, True):
                for has_late in (False, True):
                    copies = 1
                    if xx == 0 and ahead and is_first:
                        copies -= 1
                    if xx == 1 and is_first:
                        copies += 1
                    if has_late:
                        copies += 2 * len({0: () if ahead else (0,), 1: (0, 1)}.get(xx, (xx,)))
                    if copies:

                        @pl.when(
                            (x == xx)
                            & (first_head == is_first)
                            & ((late >= heads) == has_late)
                        )
                        def _(copies=copies):
                            left(many(copies * OUT_ROWS), f_send)

    load_all.wait()

    @pl.when(core == 0)
    def _():
        for some in (far_ones, [*near_ones, 0]):
            for n in range(HALVES):
                for d in some:
                    part_copy(n, d).start()
        load_ids.wait()
        ids_copy().start()
        spec_out[...] = local_spectrum()
        spec_copy().start()

    @pl.when(core == 1)
    def _():
        for some in (far_ones, near_ones):
            for n in range(HALVES):
                for d in some:
                    part_copy(n, d).start()

        first = lax.broadcasted_iota(jnp.int32, (snaps, LANES), 0) < half

        def spread_shells(c):
            for g in range(GROUPS):
                if c == 1:
                    row = all_ids[pl.ds(me * GROUPS + g, 1), :]
                else:
                    row = peer_ids[c // 2, g : g + 1, :]
                row = jnp.broadcast_to(row, (SHELLS, LANES))
                hot = jnp.where(row == shells, 1.0, 0.0).astype(jnp.bfloat16)
                onehot[c, :, g * LANES : (g + 1) * LANES] = hot

        def widen(core_of, n):
            for t in range(snaps):
                for c in range(3):
                    value = recv[core_of, n, t, c].astype(jnp.float32)
                    for at in (t, t + snaps) if t < half else (t,):
                        row = at * PITCH + n * PIECE
                        wide[c, row : row + PIECE, :] = value

        def products(g):
            def rows(c, p, d):
                return wide[c, pl.ds(d * PITCH + 2 * g + p, snaps, stride=PITCH), :]

            def put(k, value):
                terms[k * snaps : (k + 1) * snaps, g * LANES : (g + 1) * LANES] = value.astype(
                    jnp.bfloat16
                )

            own = [[rows(c, p, 0) for p in range(2)] for c in range(3)]
            for d in range(1, half + 1):
                other = [[rows(c, p, d) for p in range(2)] for c in range(3)]
                real = sum(own[c][p] * other[c][p] for c in range(3) for p in range(2))
                imag = sum(own[c][1] * other[c][0] - own[c][0] * other[c][1] for c in range(3))
                if d < half:
                    put(2 * d - 2, real)
                    put(2 * d - 1, imag)
                else:
                    put(2 * d - 2, jnp.where(first, real, imag))

        def bin_part(core_of, q):
            for g in (2 * q, 2 * q + 1):
                products(g)
            modes = slice(2 * q * LANES, 2 * (q + 1) * LANES)
            return lax.dot_general(
                terms[:, modes],
                onehot[core_of, :, modes],
                (((1,), (1,)), ((), ())),
                preferred_element_type=jnp.float32,
            )

        with jax.named_scope("c_onehot"):
            load_ids.wait()
            spread_shells(1)

            @pl.when(z_hi < heads)
            def _():
                arrived(peer_ids.at[0], i_recv.at[0])
                spread_shells(0)

        with jax.named_scope("c_spectrum"):
            mine = local_spectrum()
            spec_copy().wait_recv()
            spec_x[x] = mine + spec_peer[...]
            for d in x_steps:
                remote(
                    spec_x.at[x],
                    spec_x.at[x],
                    t_send,
                    t_rsem,
                    me,
                    slab_of((x + d) % x_n, z_hi, 1),
                ).start()

        quarters = GROUPS // 2 // HALVES

        def work_off(c, n):
            with jax.named_scope(f"d_wait{c}{n}"):
                arrived(recv.at[c, n], m_recv.at[c, n])
            with jax.named_scope(f"e_work{c}{n}"):
                widen(c, n)
                for q in range(n * quarters, (n + 1) * quarters):
                    if (c, q) == (1, 0):
                        binned[...] = bin_part(c, q)
                    else:
                        binned[...] += bin_part(c, q)

        for n in range(HALVES):
            work_off(1, n)

            @pl.when(z_hi < heads)
            def _(n=n):
                work_off(0, n)

        @pl.when((z_hi < heads) & (late >= heads))
        def _():
            arrived(peer_ids.at[1], i_recv.at[1])
            spread_shells(2)
            for n in range(HALVES):
                work_off(2, n)

        with jax.named_scope("g_turn"):
            for k in range(snaps - 1):
                value, shift = binned[k * snaps : (k + 1) * snaps], (k // 2 + 1) // 2
                sums[pl.ds(shift * snaps + k, snaps - shift, stride=snaps), :] = value[
                    0 : snaps - shift
                ]
                if shift:
                    sums[pl.ds(k, shift, stride=snaps), :] = value[snaps - shift :]
            sums[pl.ds(snaps - 1, snaps, stride=snaps), :] = jnp.zeros((snaps, SHELLS), jnp.float32)

        with jax.named_scope("h_owner"):
            for d in y_steps:
                yy = (y + d) % y_n
                remote(
                    sums.at[rows_of(yy, block)],
                    r_recv.at[y],
                    r_send,
                    r_rsem,
                    yy * Z_LO + z_lo,
                    slab,
                ).start()
            r_recv[y] = sums[rows_of(y, block), :]
            if x_n > 1:
                arrived(spec_x.at[pl.ds(0, x_n - 1)], t_rsem)
            spec_recv[me] = ordered_sum([spec_x[i] for i in range(x_n)])
            for d in by_distance:
                remote(
                    spec_recv.at[me], spec_recv.at[me], s_send, s_rsem, there(d), slab
                ).start()
            arrived(r_recv.at[pl.ds(0, y_n - 1)], r_rsem)
            x_recv[x] = ordered_sum([r_recv[i] for i in range(y_n)])

        with jax.named_scope("i_x"):
            for d in x_steps:
                remote(
                    x_recv.at[x],
                    x_recv.at[x],
                    x_send,
                    x_rsem,
                    me,
                    slab_of((x + d) % x_n, z_hi, 1),
                ).start()
            if x_n > 1:
                arrived(x_recv.at[pl.ds(0, x_n - 1)], x_rsem)
            total = ordered_sum([x_recv[i] for i in range(x_n)])
            arrived(spec_recv.at[pl.ds(0, snaps - 1)], s_rsem)

        with jax.named_scope("j_pairs"):
            for t in range(snaps):
                own_src[t : t + 1, :] = spec_recv[t]
            for k in range(Z_LO):
                for d in range(1, half + 1):
                    row = k * snaps + 2 * d - 2
                    pair_src[k, d - 1] = total[row : row + 2]

        def pair_copy(h, k, i, send_sem, recv_sem):
            count = len(pairs_at[i])
            return remote(
                pair_src.at[k, pl.ds(pairs_at[i][0] - 1, count)],
                pair_recv.at[z, slots.index(i), pl.ds(0, count)],
                send_sem,
                recv_sem,
                (base + snaps + k + i) % snaps,
                slab_of(x, h, 1),
            )

        with jax.named_scope("k_send"):
            for h in range(heads):
                for k, i in away:
                    pair_copy(h, k, i, p_send, p_rsem).start()
                for k, i in at_home:
                    here = (z_hi == h) & (z_lo == k + i)

                    @pl.when(here)
                    def _(k=k, i=i):
                        first_pair, count = pairs_at[i][0] - 1, len(pairs_at[i])
                        pair_recv[z, slots.index(i), 0:count] = pair_src[
                            k, first_pair : first_pair + count
                        ]

                    @pl.when(jnp.logical_not(here))
                    def _(h=h, k=k, i=i):
                        pair_copy(h, k, i, h_send, h_rsem).start()

                @pl.when(z_hi != h)
                def _(h=h):
                    remote(
                        own_src, own_recv.at[z_hi], o_send, o_rsem, me, slab_of(x, h, 1)
                    ).start()

                @pl.when(z_hi == h)
                def _(h=h):
                    own_recv[h] = own_src[...]

        @pl.when(z_hi < heads)
        def _():
            with jax.named_scope("l_pairwait"):
                arrived(many(z_n * away_rows // Z_LO), p_rsem)
                arrived(home_rows(z_n - 1), h_rsem)
                if z_hi_n > 1:
                    arrived(own_recv.at[pl.ds(0, z_hi_n - 1)], o_rsem)

            with jax.named_scope("m_coh"):
                load_order.wait()
                own = ordered_sum([own_recv[h] for h in range(z_hi_n)])
                for t in range(snaps):
                    spec_rows[t] = own[t : t + 1]
                spec = spec_rows[me]
                final[snaps : snaps + 1, :] = spec

                def pair(i, d):
                    at = pairs_at[i].index(d)
                    return ordered_sum([pair_recv[p, slots.index(i), at] for p in range(z_n)])

                def power(rows):
                    re, im = rows[0:1], rows[1:2]
                    return re * re + im * im

                def put_row(e, value):
                    coh_rows[e] = value / (spec * spec_rows[(me + snaps - e) % snaps])

                put_row(0, spec * spec)
                for d in range(1, half):
                    put_row(d, power(pair((d + 1) // 2, d)))
                    put_row(snaps - d, power(pair(-(d // 2), d)))
                re = pair((half + 1) // 2, half)[0:1]
                im = pair(-(half // 2), half)[0:1]
                put_row(half, re * re + im * im)
                for j in range(snaps):
                    final[j : j + 1, :] = coh_rows[(me - order_ref[j] + snaps) % snaps]
                forward_all()

        @pl.when(z_hi >= heads)
        def _():
            with jax.named_scope("n_finalwait"):
                arrived(final, f_rsem)
                load_order.wait()

    @pl.when(core == 0)
    def _():
        with jax.named_scope("n_finalwait"):
            arrived(final, f_rsem)

    with jax.named_scope("o_end"):
        out_ref[...] = final[0 : snaps + 1]
        @pl.when(core == 0)
        def _():
            left(src, m_send)
            left(peer_ids.at[0], i_send)
            left(spec_out, e_send)

        @pl.when(core == 1)
        def _():
            left(src.at[:, pl.ds(0, (snaps - 1) * ROWS)], m_send)
            left(r_recv.at[pl.ds(0, y_n - 1)], r_send)
            if x_n > 1:
                left(x_recv.at[pl.ds(0, x_n - 1)], x_send)
                left(spec_x.at[pl.ds(0, x_n - 1)], t_send)
            left(spec_recv.at[pl.ds(0, snaps - 1)], s_send)
            left(many(heads * away_rows), p_send)

            @pl.when(z_hi < heads)
            def _():
                left(home_rows(heads * Z_LO - 1), h_send)
                if heads > 1:
                    left(own_recv.at[pl.ds(0, heads - 1)], o_send)
                forwards_left()

            @pl.when(z_hi >= heads)
            def _():
                left(home_rows(heads * Z_LO), h_send)
                left(own_recv.at[pl.ds(0, heads)], o_send)


def finish(snaps, done_ref, coh_ref, spec_ref, sem):
    coh = pltpu.make_async_copy(done_ref.at[0:snaps], coh_ref.at[0], sem.at[0])
    spec = pltpu.make_async_copy(done_ref.at[snaps : snaps + 1], spec_ref, sem.at[1])
    coh.start()
    spec.start()
    coh.wait()
    spec.wait()


def body(sizes, velocity, shell_index, ref_order):
    snaps, x_n, z_hi_n = sizes
    half = snaps // 2
    heads = min(2, z_hi_n)
    lanes_n = velocity.shape[3] // LANES
    vel = velocity.reshape(3, 2, lanes_n, LANES).transpose(0, 2, 1, 3)
    vel = vel.reshape(3, 2 * lanes_n, LANES)
    ids = shell_index.reshape(lanes_n, LANES)
    f32, bf16, dma = jnp.float32, jnp.bfloat16, pltpu.SemaphoreType.DMA
    done = pl.pallas_call(
        functools.partial(kernel, sizes),
        out_shape=pltpu.VMEM((snaps + 1, SHELLS), f32),
        in_specs=[pl.BlockSpec(memory_space=pl.ANY)] * 3,
        out_specs=pl.BlockSpec(memory_space=pltpu.VMEM),
        scratch_shapes=[
            pltpu.VMEM((3, 2 * lanes_n, LANES), bf16),
            pltpu.VMEM((SETS, HALVES, snaps, 3, PIECE, LANES), bf16),
            pltpu.VMEM((lanes_n, LANES), jnp.int32),
            pltpu.VMEM((2, GROUPS, LANES), jnp.int32),
            pltpu.SMEM((snaps,), jnp.int32),
            pltpu.VMEM((3, (snaps + half + 1) * PITCH, LANES), f32),
            pltpu.VMEM(((snaps - 1) * snaps, GROUPS * LANES), bf16),
            pltpu.VMEM((SETS, SHELLS, GROUPS * LANES), bf16),
            pltpu.VMEM(((snaps - 1) * snaps, SHELLS), f32),
            pltpu.VMEM((snaps * snaps, SHELLS), f32),
            pltpu.VMEM((snaps // Z_LO, Z_LO * snaps, SHELLS), f32),
            pltpu.VMEM((x_n, Z_LO * snaps, SHELLS), f32),
            pltpu.VMEM((1, SHELLS), f32),
            pltpu.VMEM((1, SHELLS), f32),
            pltpu.VMEM((x_n, 1, SHELLS), f32),
            pltpu.VMEM((snaps, 1, SHELLS), f32),
            pltpu.VMEM((snaps, SHELLS), f32),
            pltpu.VMEM((z_hi_n, snaps, SHELLS), f32),
            pltpu.VMEM((Z_LO, half, 2, SHELLS), f32),
            pltpu.VMEM((z_hi_n * Z_LO, half + 1, 2, 2, SHELLS), f32),
            pltpu.VMEM((snaps, 1, SHELLS), f32),
            pltpu.VMEM((snaps, 1, SHELLS), f32),
            pltpu.VMEM((OUT_ROWS, SHELLS), f32),
            dma((3,)),
            dma(()),
            dma((SETS, HALVES)),
            dma(()),
            dma((2,)),
            *[dma(())] * 18,
        ],
        compiler_params=pltpu.CompilerParams(collective_id=0, has_side_effects=True),
    )(vel, ids, ref_order)
    return pl.pallas_call(
        functools.partial(finish, snaps),
        out_shape=(
            jax.ShapeDtypeStruct((1, snaps, SHELLS), f32),
            jax.ShapeDtypeStruct((1, SHELLS), f32),
        ),
        in_specs=[pl.BlockSpec(memory_space=pltpu.VMEM)],
        out_specs=(pl.BlockSpec(memory_space=pl.ANY),) * 2,
        scratch_shapes=[dma((2,))],
    )(pltpu.with_memory_space_constraint(done, pltpu.VMEM))


def solution(mesh):
    snaps, slabs = mesh.shape["tm"], mesh.shape["slab"]
    z_hi_n = min(Z_HI, slabs // CORES)
    sizes = (snaps, slabs // CORES // z_hi_n, z_hi_n)
    return jax.shard_map(
        functools.partial(body, sizes),
        mesh=mesh,
        in_specs=(P("tm", None, None, "slab"), P("slab"), P()),
        out_specs=(P("tm", None, None), P("tm", None)),
        check_vma=False,
    )
```

```python
import functools

import jax
import jax.numpy as jnp
from jax import lax
from jax.experimental import pallas as pl
from jax.experimental.pallas import tpu as pltpu
from jax.sharding import PartitionSpec as P

SHELLS = 128
LANES = 128
Z_LO, Z_HI, CORES = 2, 4, 2
ROWS = 16
GROUPS = ROWS // 2
PITCH = ROWS + 1
SETS = 3
HALVES = 2
PIECE = ROWS // HALVES
OUT_ROWS = 24


def remote(src, dst, send_sem, recv_sem, tm, slab):
    return pltpu.make_async_remote_copy(
        src_ref=src,
        dst_ref=dst,
        send_sem=send_sem,
        recv_sem=recv_sem,
        device_id={"tm": tm, "slab": slab},
        device_id_type=pl.DeviceIdType.MESH,
    )


def arrived(ref, sem):
    remote(ref, ref, sem, sem, lax.axis_index("tm"), lax.axis_index("slab")).wait_recv()


def left(ref, sem):
    remote(ref, ref, sem, sem, lax.axis_index("tm"), lax.axis_index("slab")).wait_send()


def ordered_sum(terms):
    total = terms[0]
    for term in terms[1:]:
        total = total + term
    return total


def kernel(
    sizes,
    vel_ref,
    shell_ref,
    order_hbm,
    out_ref,
    src,
    recv,
    all_ids,
    peer_ids,
    order_ref,
    wide,
    terms,
    onehot,
    binned,
    sums,
    r_recv,
    x_recv,
    spec_out,
    spec_peer,
    spec_x,
    spec_recv,
    own_src,
    own_recv,
    pair_src,
    pair_recv,
    spec_rows,
    power_rows,
    coh_rows,
    final,
    load_sem,
    m_send,
    m_recv,
    i_send,
    i_recv,
    r_send,
    r_rsem,
    x_send,
    x_rsem,
    p_send,
    p_rsem,
    h_send,
    h_rsem,
    o_send,
    o_rsem,
    e_send,
    e_rsem,
    s_send,
    s_rsem,
    t_send,
    t_rsem,
    f_send,
    f_rsem,
):
    snaps, x_n, z_hi_n = sizes
    half = snaps // 2
    heads = min(2, z_hi_n)
    me = lax.axis_index("tm")
    slab = lax.axis_index("slab")
    core = slab % CORES
    x, z_hi = slab // CORES // z_hi_n, slab // CORES % z_hi_n
    y_n, z_n = snaps // Z_LO, z_hi_n * Z_LO
    y, z_lo = me // Z_LO, me % Z_LO
    z = z_hi * Z_LO + z_lo
    base = y * Z_LO
    block = Z_LO * snaps
    far = slab - core
    near = far + 1
    late = z_hi_n - 1 - z_hi
    is_late = z_hi // heads
    part_set = core + (1 - core) * 2 * is_late
    by_distance = sorted(range(1, snaps), key=lambda d: (-min(d, snaps - d), d))
    far_ones, near_ones = by_distance[: half - 2], by_distance[half - 2 :]

    pairs_at = {0: (1,)}
    for step in range(1, (half + 1) // 2 + 1):
        pairs_at[step] = tuple(d for d in (2 * step - 1, 2 * step) if d <= half)
    for step in range(1, half // 2 + 1):
        pairs_at[-step] = tuple(d for d in (2 * step, 2 * step + 1) if d <= half)
    y_steps = sorted(range(1, y_n), key=lambda d: -min(d, y_n - d))
    x_steps = sorted(range(1, x_n), key=lambda d: -min(d, x_n - d))
    messages = sorted(
        ((k, i) for k in range(Z_LO) for i in pairs_at), key=lambda m: (-abs(m[1]), m)
    )
    away = [(k, i) for k, i in messages if not 0 <= k + i < Z_LO]
    at_home = [(k, i) for k, i in messages if 0 <= k + i < Z_LO]
    away_rows = sum(2 * len(pairs_at[i]) for _, i in away)
    reach = sorted({k + i for k, i in messages})
    slots = list(pairs_at)

    def there(d):
        return (me + d) % snaps

    def whence(d):
        return (me + snaps - d) % snaps

    def slab_of(xx, zz, cc):
        return (xx * z_hi_n + zz) * CORES + cc

    def many(n):
        if n <= r_recv.shape[1]:
            return r_recv.at[0, pl.ds(0, n)]
        if 2 * n > vel_ref.shape[1]:
            return vel_ref.at[pl.ds(0, 2), pl.ds(0, n)]
        return vel_ref.at[0, pl.ds(0, 2 * n)]

    def home_rows(n):
        return pair_recv.at[pl.ds(0, n), pl.ds(0, 3), 0]

    def rows_of(t, n):
        return pl.ds(pl.multiple_of(t * n, n), n)

    load_all = pltpu.make_async_copy(vel_ref, src, load_sem.at[0])
    load_all.start()
    load_ids = pltpu.make_async_copy(shell_ref, all_ids, load_sem.at[1])
    load_ids.start()
    load_own = [
        pltpu.make_async_copy(
            vel_ref.at[:, pl.ds(pl.multiple_of(me * ROWS + n * PIECE, PIECE), PIECE)],
            recv.at[1, n, me],
            m_recv.at[1, n],
        )
        for n in range(HALVES)
    ]
    load_order = pltpu.make_async_copy(order_hbm, order_ref, load_sem.at[2])

    barrier = pltpu.get_barrier_semaphore()

    def greet(tm, sl):
        pl.semaphore_signal(
            barrier, inc=1, device_id={"tm": tm, "slab": sl}, device_id_type=pl.DeviceIdType.MESH
        )

    with jax.named_scope("a_greet"):

        @pl.when(core == 1)
        def _():
            @pl.when(z_hi < heads)
            def _():
                @pl.when(late >= heads)
                def _():
                    for d in [*by_distance, 0]:
                        greet(there(d), slab_of(x, late, 0))

                for d in by_distance:
                    greet(there(d), near)
                    greet(there(d), far)

            @pl.when(z_hi >= heads)
            def _():
                for d in by_distance:
                    greet(there(d), near)

            greet(me, far)
            for d in range(1, x_n):
                greet(there(0), slab_of((x + d) % x_n, z_hi, 1))

        @pl.when(core == 1)
        def _():
            for copy in load_own:
                copy.start()
            load_order.start()

            @pl.when(z_hi < heads)
            def _():
                for h in range(1, z_hi_n):
                    for i in reach:
                        greet((base + snaps + i) % snaps, slab_of(x, (z_hi + h) % z_hi_n, 1))

    with jax.named_scope("b_barrier"):

        @pl.when(core == 0)
        def _():
            @pl.when(z_hi < heads)
            def _():
                pl.semaphore_wait(barrier, snaps)

            @pl.when(z_hi >= heads)
            def _():
                pl.semaphore_wait(barrier, snaps + 1)

        @pl.when(core == 1)
        def _():
            @pl.when(z_hi < heads)
            def _():
                pl.semaphore_wait(barrier, snaps - 1 + x_n - 1 + (heads - 1) * len(reach))

            @pl.when(z_hi >= heads)
            def _():
                pl.semaphore_wait(barrier, snaps - 1 + x_n - 1 + heads * len(reach))

    def part_copy(n, d):
        return remote(
            src.at[:, pl.ds(pl.multiple_of(there(d) * ROWS + n * PIECE, PIECE), PIECE)],
            recv.at[part_set, n, me],
            m_send,
            m_recv.at[part_set, n],
            there(d),
            slab_of(x, z_hi + (1 - core) * is_late * (late - z_hi), 1),
        )

    def ids_copy():
        return remote(
            all_ids.at[rows_of(me, GROUPS)],
            peer_ids.at[is_late],
            i_send,
            i_recv.at[is_late],
            me,
            slab_of(x, z_hi + is_late * (late - z_hi), 1),
        )

    def spec_copy():
        return remote(spec_out, spec_peer, e_send, e_rsem, me, near)

    shells = lax.broadcasted_iota(jnp.int32, (SHELLS, LANES), 0)

    def local_spectrum():
        lanes_n = shell_ref.shape[0]
        squares = ordered_sum([src[c].astype(jnp.float32) ** 2 for c in range(3)])
        wide[0, 0 : 2 * lanes_n, :] = squares
        energy = wide[0, pl.ds(0, lanes_n, stride=2), :] + wide[0, pl.ds(1, lanes_n, stride=2), :]
        wide[1, 0:lanes_n, :] = energy.astype(jnp.bfloat16).astype(jnp.float32)

        def add_rows(i, total):
            at = rows_of(i, 8)
            shell, value = all_ids[at, :], wide[1, at, :]
            for r in range(8):
                hit = jnp.broadcast_to(shell[r : r + 1], (SHELLS, LANES)) == shells
                total = total + jnp.where(
                    hit, jnp.broadcast_to(value[r : r + 1], (SHELLS, LANES)), 0.0
                )
            return total

        by_lane = lax.fori_loop(
            0, lanes_n // 8, add_rows, jnp.zeros((SHELLS, LANES), jnp.float32)
        )
        return lax.dot_general(
            jnp.ones((8, LANES), jnp.float32),
            by_lane,
            (((1,), (1,)), ((), ())),
            precision=lax.Precision.HIGHEST,
            preferred_element_type=jnp.float32,
        )[0:1]

    ahead = 1 if x_n > 1 else 0
    first_head = (me == 0) & (z_hi == 0)

    def forward(xx, zz, c):
        remote(final, final, f_send, f_rsem, me, slab_of(xx, zz, c)).start()

    def forward_all():
        for xx in range(x_n):

            @pl.when(x == xx)
            def _(xx=xx):
                if xx or not ahead:
                    forward(xx, z_hi, 0)
                else:

                    @pl.when(jnp.logical_not(first_head))
                    def _():
                        forward(xx, z_hi, 0)

                if xx == ahead and xx:

                    @pl.when(first_head)
                    def _():
                        forward(0, z_hi, 0)

                @pl.when(late >= heads)
                def _():
                    for to in {0: () if ahead else (0,), 1: (0, 1)}.get(xx, (xx,)):
                        forward(to, late, 1)
                        forward(to, late, 0)

    def forwards_left():
        for xx in range(x_n):
            for is_first in (False, True):
                for has_late in (False, True):
                    copies = 1
                    if xx == 0 and ahead and is_first:
                        copies -= 1
                    if xx == 1 and is_first:
                        copies += 1
                    if has_late:
                        copies += 2 * len({0: () if ahead else (0,), 1: (0, 1)}.get(xx, (xx,)))
                    if copies:

                        @pl.when(
                            (x == xx)
                            & (first_head == is_first)
                            & ((late >= heads) == has_late)
                        )
                        def _(copies=copies):
                            left(many(copies * OUT_ROWS), f_send)

    load_all.wait()

    @pl.when(core == 0)
    def _():
        for some in (far_ones, [*near_ones, 0]):
            for n in range(HALVES):
                for d in some:
                    part_copy(n, d).start()
        load_ids.wait()
        ids_copy().start()
        spec_out[...] = local_spectrum()
        spec_copy().start()

    @pl.when(core == 1)
    def _():
        for some in (far_ones, near_ones):
            for n in range(HALVES):
                for d in some:
                    part_copy(n, d).start()

        first = lax.broadcasted_iota(jnp.int32, (snaps, LANES), 0) < half

        def spread_shells(c):
            for g in range(GROUPS):
                if c == 1:
                    row = all_ids[pl.ds(me * GROUPS + g, 1), :]
                else:
                    row = peer_ids[c // 2, g : g + 1, :]
                row = jnp.broadcast_to(row, (SHELLS, LANES))
                hot = jnp.where(row == shells, 1.0, 0.0).astype(jnp.bfloat16)
                onehot[c, :, g * LANES : (g + 1) * LANES] = hot

        def widen(core_of, n):
            for t in range(snaps):
                for c in range(3):
                    value = recv[core_of, n, t, c].astype(jnp.float32)
                    for at in (t, t + snaps) if t < half else (t,):
                        row = at * PITCH + n * PIECE
                        wide[c, row : row + PIECE, :] = value

        def products(g):
            def rows(c, p, d):
                return wide[c, pl.ds(d * PITCH + 2 * g + p, snaps, stride=PITCH), :]

            def put(k, value):
                terms[k * snaps : (k + 1) * snaps, g * LANES : (g + 1) * LANES] = value.astype(
                    jnp.bfloat16
                )

            own = [[rows(c, p, 0) for p in range(2)] for c in range(3)]
            for d in range(1, half + 1):
                other = [[rows(c, p, d) for p in range(2)] for c in range(3)]
                real = sum(own[c][p] * other[c][p] for c in range(3) for p in range(2))
                imag = sum(own[c][1] * other[c][0] - own[c][0] * other[c][1] for c in range(3))
                if d < half:
                    put(2 * d - 2, real)
                    put(2 * d - 1, imag)
                else:
                    put(2 * d - 2, jnp.where(first, real, imag))

        def bin_part(core_of, q):
            for g in (2 * q, 2 * q + 1):
                products(g)
            modes = slice(2 * q * LANES, 2 * (q + 1) * LANES)
            return lax.dot_general(
                terms[:, modes],
                onehot[core_of, :, modes],
                (((1,), (1,)), ((), ())),
                preferred_element_type=jnp.float32,
            )

        with jax.named_scope("c_onehot"):
            load_ids.wait()
            spread_shells(1)

            @pl.when(z_hi < heads)
            def _():
                arrived(peer_ids.at[0], i_recv.at[0])
                spread_shells(0)

        with jax.named_scope("c_spectrum"):
            mine = local_spectrum()
            spec_copy().wait_recv()
            spec_x[x] = mine + spec_peer[...]
            for d in x_steps:
                remote(
                    spec_x.at[x],
                    spec_x.at[x],
                    t_send,
                    t_rsem,
                    me,
                    slab_of((x + d) % x_n, z_hi, 1),
                ).start()

        quarters = GROUPS // 2 // HALVES

        def work_off(c, n):
            with jax.named_scope(f"d_wait{c}{n}"):
                arrived(recv.at[c, n], m_recv.at[c, n])
            with jax.named_scope(f"e_work{c}{n}"):
                widen(c, n)
                for q in range(n * quarters, (n + 1) * quarters):
                    if (c, q) == (1, 0):
                        binned[...] = bin_part(c, q)
                    else:
                        binned[...] += bin_part(c, q)

        for n in range(HALVES):
            work_off(1, n)

            @pl.when(z_hi < heads)
            def _(n=n):
                work_off(0, n)

        @pl.when((z_hi < heads) & (late >= heads))
        def _():
            arrived(peer_ids.at[1], i_recv.at[1])
            spread_shells(2)
            for n in range(HALVES):
                work_off(2, n)

        with jax.named_scope("g_turn"):
            for k in range(snaps - 1):
                value, shift = binned[k * snaps : (k + 1) * snaps], (k // 2 + 1) // 2
                sums[pl.ds(shift * snaps + k, snaps - shift, stride=snaps), :] = value[
                    0 : snaps - shift
                ]
                if shift:
                    sums[pl.ds(k, shift, stride=snaps), :] = value[snaps - shift :]
            sums[pl.ds(snaps - 1, snaps, stride=snaps), :] = jnp.zeros((snaps, SHELLS), jnp.float32)

        with jax.named_scope("h_owner"):
            for d in y_steps:
                yy = (y + d) % y_n
                remote(
                    sums.at[rows_of(yy, block)],
                    r_recv.at[y],
                    r_send,
                    r_rsem,
                    yy * Z_LO + z_lo,
                    slab,
                ).start()
            r_recv[y] = sums[rows_of(y, block), :]
            if x_n > 1:
                arrived(spec_x.at[pl.ds(0, x_n - 1)], t_rsem)
            spec_recv[me] = ordered_sum([spec_x[i] for i in range(x_n)])
            for d in by_distance:
                remote(
                    spec_recv.at[me], spec_recv.at[me], s_send, s_rsem, there(d), slab
                ).start()
            arrived(r_recv.at[pl.ds(0, y_n - 1)], r_rsem)
            x_recv[x] = ordered_sum([r_recv[i] for i in range(y_n)])

        with jax.named_scope("i_x"):
            for d in x_steps:
                remote(
                    x_recv.at[x],
                    x_recv.at[x],
                    x_send,
                    x_rsem,
                    me,
                    slab_of((x + d) % x_n, z_hi, 1),
                ).start()
            arrived(spec_recv.at[pl.ds(0, snaps - 1)], s_rsem)
            for t in range(snaps):
                own_src[t : t + 1, :] = spec_recv[t]
            for h in range(heads):

                @pl.when(z_hi != h)
                def _(h=h):
                    remote(
                        own_src, own_recv.at[z_hi], o_send, o_rsem, me, slab_of(x, h, 1)
                    ).start()

                @pl.when(z_hi == h)
                def _(h=h):
                    own_recv[h] = own_src[...]

            if x_n > 1:
                arrived(x_recv.at[pl.ds(0, x_n - 1)], x_rsem)
            total = ordered_sum([x_recv[i] for i in range(x_n)])

        with jax.named_scope("j_pairs"):
            for k in range(Z_LO):
                for d in range(1, half + 1):
                    row = k * snaps + 2 * d - 2
                    pair_src[k, d - 1] = total[row : row + 2]

        def pair_copy(h, k, i, send_sem, recv_sem):
            count = len(pairs_at[i])
            return remote(
                pair_src.at[k, pl.ds(pairs_at[i][0] - 1, count)],
                pair_recv.at[z, slots.index(i), pl.ds(0, count)],
                send_sem,
                recv_sem,
                (base + snaps + k + i) % snaps,
                slab_of(x, h, 1),
            )

        with jax.named_scope("k_send"):
            for h in range(heads):
                for k, i in away:
                    pair_copy(h, k, i, p_send, p_rsem).start()
                for k, i in at_home:
                    here = (z_hi == h) & (z_lo == k + i)

                    @pl.when(here)
                    def _(k=k, i=i):
                        first_pair, count = pairs_at[i][0] - 1, len(pairs_at[i])
                        pair_recv[z, slots.index(i), 0:count] = pair_src[
                            k, first_pair : first_pair + count
                        ]

                    @pl.when(jnp.logical_not(here))
                    def _(h=h, k=k, i=i):
                        pair_copy(h, k, i, h_send, h_rsem).start()

        left(src.at[:, pl.ds(0, (snaps - 1) * ROWS)], m_send)
        left(r_recv.at[pl.ds(0, y_n - 1)], r_send)
        if x_n > 1:
            left(x_recv.at[pl.ds(0, x_n - 1)], x_send)
            left(spec_x.at[pl.ds(0, x_n - 1)], t_send)
        left(spec_recv.at[pl.ds(0, snaps - 1)], s_send)

        @pl.when(z_hi < heads)
        def _():
            with jax.named_scope("l_pairwait"):
                arrived(many(z_n * away_rows // Z_LO), p_rsem)
                arrived(home_rows(z_n - 1), h_rsem)
                if z_hi_n > 1:
                    arrived(own_recv.at[pl.ds(0, z_hi_n - 1)], o_rsem)

            with jax.named_scope("m_coh"):
                load_order.wait()
                own = ordered_sum([own_recv[h] for h in range(z_hi_n)])
                spec_rows[...] = own
                spec = spec_rows[pl.ds(me, 1), :]
                final[snaps : snaps + 1, :] = spec

                def pair(i, d):
                    at = pairs_at[i].index(d)
                    return ordered_sum([pair_recv[p, slots.index(i), at] for p in range(z_n)])

                def power(rows):
                    re, im = rows[0:1], rows[1:2]
                    return re * re + im * im

                def put_row(e, value):
                    power_rows[pl.ds((me + snaps - e) % snaps, 1), :] = value

                put_row(0, spec * spec)
                for d in range(1, half):
                    put_row(d, power(pair((d + 1) // 2, d)))
                    put_row(snaps - d, power(pair(-(d // 2), d)))
                re = pair((half + 1) // 2, half)[0:1]
                im = pair(-(half // 2), half)[0:1]
                put_row(half, re * re + im * im)
                coh_rows[...] = power_rows[...] / (spec * own)
                for j in range(snaps):
                    final[j : j + 1, :] = coh_rows[pl.ds(order_ref[j], 1), :]
                forward_all()

        @pl.when(z_hi >= heads)
        def _():
            with jax.named_scope("n_finalwait"):
                arrived(final, f_rsem)
                load_order.wait()

    @pl.when(core == 0)
    def _():
        with jax.named_scope("n_finalwait"):
            arrived(final, f_rsem)

    with jax.named_scope("o_end"):
        out_ref[...] = final[0 : snaps + 1]
        @pl.when(core == 0)
        def _():
            left(src, m_send)
            left(peer_ids.at[0], i_send)
            left(spec_out, e_send)

        @pl.when(core == 1)
        def _():
            left(many(heads * away_rows), p_send)

            @pl.when(z_hi < heads)
            def _():
                left(home_rows(heads * Z_LO - 1), h_send)
                if heads > 1:
                    left(own_recv.at[pl.ds(0, heads - 1)], o_send)
                forwards_left()

            @pl.when(z_hi >= heads)
            def _():
                left(home_rows(heads * Z_LO), h_send)
                left(own_recv.at[pl.ds(0, heads)], o_send)


def finish(snaps, done_ref, coh_ref, spec_ref, sem):
    coh = pltpu.make_async_copy(done_ref.at[0:snaps], coh_ref.at[0], sem.at[0])
    spec = pltpu.make_async_copy(done_ref.at[snaps : snaps + 1], spec_ref, sem.at[1])
    coh.start()
    spec.start()
    coh.wait()
    spec.wait()


def body(sizes, velocity, shell_index, ref_order):
    snaps, x_n, z_hi_n = sizes
    half = snaps // 2
    heads = min(2, z_hi_n)
    lanes_n = velocity.shape[3] // LANES
    vel = velocity.reshape(3, 2, lanes_n, LANES).transpose(0, 2, 1, 3)
    vel = vel.reshape(3, 2 * lanes_n, LANES)
    ids = shell_index.reshape(lanes_n, LANES)
    f32, bf16, dma = jnp.float32, jnp.bfloat16, pltpu.SemaphoreType.DMA
    done = pl.pallas_call(
        functools.partial(kernel, sizes),
        out_shape=pltpu.VMEM((snaps + 1, SHELLS), f32),
        in_specs=[pl.BlockSpec(memory_space=pl.ANY)] * 3,
        out_specs=pl.BlockSpec(memory_space=pltpu.VMEM),
        scratch_shapes=[
            pltpu.VMEM((3, 2 * lanes_n, LANES), bf16),
            pltpu.VMEM((SETS, HALVES, snaps, 3, PIECE, LANES), bf16),
            pltpu.VMEM((lanes_n, LANES), jnp.int32),
            pltpu.VMEM((2, GROUPS, LANES), jnp.int32),
            pltpu.SMEM((snaps,), jnp.int32),
            pltpu.VMEM((3, (snaps + half + 1) * PITCH, LANES), f32),
            pltpu.VMEM(((snaps - 1) * snaps, GROUPS * LANES), bf16),
            pltpu.VMEM((SETS, SHELLS, GROUPS * LANES), bf16),
            pltpu.VMEM(((snaps - 1) * snaps, SHELLS), f32),
            pltpu.VMEM((snaps * snaps, SHELLS), f32),
            pltpu.VMEM((snaps // Z_LO, Z_LO * snaps, SHELLS), f32),
            pltpu.VMEM((x_n, Z_LO * snaps, SHELLS), f32),
            pltpu.VMEM((1, SHELLS), f32),
            pltpu.VMEM((1, SHELLS), f32),
            pltpu.VMEM((x_n, 1, SHELLS), f32),
            pltpu.VMEM((snaps, 1, SHELLS), f32),
            pltpu.VMEM((snaps, SHELLS), f32),
            pltpu.VMEM((z_hi_n, snaps, SHELLS), f32),
            pltpu.VMEM((Z_LO, half, 2, SHELLS), f32),
            pltpu.VMEM((z_hi_n * Z_LO, half + 1, 2, 2, SHELLS), f32),
            pltpu.VMEM((snaps, SHELLS), f32),
            pltpu.VMEM((snaps, SHELLS), f32),
            pltpu.VMEM((snaps, SHELLS), f32),
            pltpu.VMEM((OUT_ROWS, SHELLS), f32),
            dma((3,)),
            dma(()),
            dma((SETS, HALVES)),
            dma(()),
            dma((2,)),
            *[dma(())] * 18,
        ],
        compiler_params=pltpu.CompilerParams(collective_id=0, has_side_effects=True),
    )(vel, ids, ref_order)
    return pl.pallas_call(
        functools.partial(finish, snaps),
        out_shape=(
            jax.ShapeDtypeStruct((1, snaps, SHELLS), f32),
            jax.ShapeDtypeStruct((1, SHELLS), f32),
        ),
        in_specs=[pl.BlockSpec(memory_space=pltpu.VMEM)],
        out_specs=(pl.BlockSpec(memory_space=pl.ANY),) * 2,
        scratch_shapes=[dma((2,))],
    )(pltpu.with_memory_space_constraint(done, pltpu.VMEM))


def solution(mesh):
    snaps, slabs = mesh.shape["tm"], mesh.shape["slab"]
    z_hi_n = min(Z_HI, slabs // CORES)
    sizes = (snaps, slabs // CORES // z_hi_n, z_hi_n)
    return jax.shard_map(
        functools.partial(body, sizes),
        mesh=mesh,
        in_specs=(P("tm", None, None, "slab"), P("slab"), P()),
        out_specs=(P("tm", None, None), P("tm", None)),
        check_vma=False,
    )
```

```python
import functools

import jax
import jax.numpy as jnp
from jax import lax
from jax.experimental import pallas as pl
from jax.experimental.pallas import tpu as pltpu
from jax.sharding import PartitionSpec as P

SHELLS = 128
LANES = 128
Z_LO, Z_HI, CORES = 2, 4, 2
ROWS = 16
GROUPS = ROWS // 2
PITCH = ROWS + 1
SETS = 3
HALVES = 2
PIECE = ROWS // HALVES
OUT_ROWS = 24


def remote(src, dst, send_sem, recv_sem, tm, slab):
    return pltpu.make_async_remote_copy(
        src_ref=src,
        dst_ref=dst,
        send_sem=send_sem,
        recv_sem=recv_sem,
        device_id={"tm": tm, "slab": slab},
        device_id_type=pl.DeviceIdType.MESH,
    )


def arrived(ref, sem):
    remote(ref, ref, sem, sem, lax.axis_index("tm"), lax.axis_index("slab")).wait_recv()


def left(ref, sem):
    remote(ref, ref, sem, sem, lax.axis_index("tm"), lax.axis_index("slab")).wait_send()


def ordered_sum(terms):
    total = terms[0]
    for term in terms[1:]:
        total = total + term
    return total


def kernel(
    sizes,
    vel_ref,
    shell_ref,
    order_hbm,
    out_ref,
    src,
    recv,
    all_ids,
    peer_ids,
    order_ref,
    wide,
    terms,
    onehot,
    binned,
    sums,
    r_recv,
    x_recv,
    spec_out,
    spec_peer,
    spec_x,
    spec_recv,
    own_src,
    own_recv,
    pair_src,
    pair_recv,
    spec_rows,
    power_rows,
    coh_rows,
    final,
    load_sem,
    m_send,
    m_recv,
    i_send,
    i_recv,
    r_send,
    r_rsem,
    x_send,
    x_rsem,
    p_send,
    p_rsem,
    h_send,
    h_rsem,
    o_send,
    o_rsem,
    e_send,
    e_rsem,
    s_send,
    s_rsem,
    t_send,
    t_rsem,
    f_send,
    f_rsem,
):
    snaps, x_n, z_hi_n = sizes
    half = snaps // 2
    heads = min(2, z_hi_n)
    me = lax.axis_index("tm")
    slab = lax.axis_index("slab")
    core = slab % CORES
    x, z_hi = slab // CORES // z_hi_n, slab // CORES % z_hi_n
    y_n, z_n = snaps // Z_LO, z_hi_n * Z_LO
    y, z_lo = me // Z_LO, me % Z_LO
    z = z_hi * Z_LO + z_lo
    base = y * Z_LO
    block = Z_LO * snaps
    far = slab - core
    near = far + 1
    late = z_hi_n - 1 - z_hi
    is_late = z_hi // heads
    part_set = core + (1 - core) * 2 * is_late
    by_distance = sorted(range(1, snaps), key=lambda d: (-min(d, snaps - d), d))
    far_ones, near_ones = by_distance[: half - 2], by_distance[half - 2 :]

    pairs_at = {0: (1,)}
    for step in range(1, (half + 1) // 2 + 1):
        pairs_at[step] = tuple(d for d in (2 * step - 1, 2 * step) if d <= half)
    for step in range(1, half // 2 + 1):
        pairs_at[-step] = tuple(d for d in (2 * step, 2 * step + 1) if d <= half)
    y_steps = sorted(range(1, y_n), key=lambda d: -min(d, y_n - d))
    x_steps = sorted(range(1, x_n), key=lambda d: -min(d, x_n - d))
    messages = sorted(
        ((k, i) for k in range(Z_LO) for i in pairs_at), key=lambda m: (-abs(m[1]), m)
    )
    away = [(k, i) for k, i in messages if not 0 <= k + i < Z_LO]
    at_home = [(k, i) for k, i in messages if 0 <= k + i < Z_LO]
    away_rows = sum(2 * len(pairs_at[i]) for _, i in away)
    reach = sorted({k + i for k, i in messages})
    slots = list(pairs_at)

    def there(d):
        return (me + d) % snaps

    def whence(d):
        return (me + snaps - d) % snaps

    def slab_of(xx, zz, cc):
        return (xx * z_hi_n + zz) * CORES + cc

    def many(n):
        if n <= r_recv.shape[1]:
            return r_recv.at[0, pl.ds(0, n)]
        if 2 * n > vel_ref.shape[1]:
            return vel_ref.at[pl.ds(0, 2), pl.ds(0, n)]
        return vel_ref.at[0, pl.ds(0, 2 * n)]

    def home_rows(n):
        return pair_recv.at[pl.ds(0, n), pl.ds(0, 3), 0]

    def rows_of(t, n):
        return pl.ds(pl.multiple_of(t * n, n), n)

    load_all = pltpu.make_async_copy(vel_ref, src, load_sem.at[0])
    load_all.start()
    load_ids = pltpu.make_async_copy(shell_ref, all_ids, load_sem.at[1])
    load_ids.start()
    load_own = [
        pltpu.make_async_copy(
            vel_ref.at[:, pl.ds(pl.multiple_of(me * ROWS + n * PIECE, PIECE), PIECE)],
            recv.at[1, n, me],
            m_recv.at[1, n],
        )
        for n in range(HALVES)
    ]
    load_order = pltpu.make_async_copy(order_hbm, order_ref, load_sem.at[2])

    barrier = pltpu.get_barrier_semaphore()

    def greet(tm, sl):
        pl.semaphore_signal(
            barrier, inc=1, device_id={"tm": tm, "slab": sl}, device_id_type=pl.DeviceIdType.MESH
        )

    with jax.named_scope("a_greet"):

        @pl.when(core == 1)
        def _():
            @pl.when(z_hi < heads)
            def _():
                @pl.when(late >= heads)
                def _():
                    for d in [*by_distance, 0]:
                        greet(there(d), slab_of(x, late, 0))

                for d in by_distance:
                    greet(there(d), near)
                    greet(there(d), far)

            @pl.when(z_hi >= heads)
            def _():
                for d in by_distance:
                    greet(there(d), near)

            greet(me, far)
            for d in range(1, x_n):
                greet(there(0), slab_of((x + d) % x_n, z_hi, 1))

        @pl.when(core == 1)
        def _():
            for copy in load_own:
                copy.start()
            load_order.start()

            @pl.when(z_hi < heads)
            def _():
                for h in range(1, z_hi_n):
                    for i in reach:
                        greet((base + snaps + i) % snaps, slab_of(x, (z_hi + h) % z_hi_n, 1))

    with jax.named_scope("b_barrier"):

        @pl.when(core == 0)
        def _():
            @pl.when(z_hi < heads)
            def _():
                pl.semaphore_wait(barrier, snaps)

            @pl.when(z_hi >= heads)
            def _():
                pl.semaphore_wait(barrier, snaps + 1)

        @pl.when(core == 1)
        def _():
            @pl.when(z_hi < heads)
            def _():
                pl.semaphore_wait(barrier, snaps - 1 + x_n - 1 + (heads - 1) * len(reach))

            @pl.when(z_hi >= heads)
            def _():
                pl.semaphore_wait(barrier, snaps - 1 + x_n - 1 + heads * len(reach))

    def part_copy(n, d):
        return remote(
            src.at[:, pl.ds(pl.multiple_of(there(d) * ROWS + n * PIECE, PIECE), PIECE)],
            recv.at[part_set, n, me],
            m_send,
            m_recv.at[part_set, n],
            there(d),
            slab_of(x, z_hi + (1 - core) * is_late * (late - z_hi), 1),
        )

    def ids_copy():
        return remote(
            all_ids.at[rows_of(me, GROUPS)],
            peer_ids.at[is_late],
            i_send,
            i_recv.at[is_late],
            me,
            slab_of(x, z_hi + is_late * (late - z_hi), 1),
        )

    def spec_copy():
        return remote(spec_out, spec_peer, e_send, e_rsem, me, near)

    shells = lax.broadcasted_iota(jnp.int32, (SHELLS, LANES), 0)

    def local_spectrum():
        lanes_n = shell_ref.shape[0]
        squares = ordered_sum([src[c].astype(jnp.float32) ** 2 for c in range(3)])
        wide[0, 0 : 2 * lanes_n, :] = squares
        energy = wide[0, pl.ds(0, lanes_n, stride=2), :] + wide[0, pl.ds(1, lanes_n, stride=2), :]
        wide[1, 0:lanes_n, :] = energy.astype(jnp.bfloat16).astype(jnp.float32)

        def add_rows(i, total):
            at = rows_of(i, 8)
            shell, value = all_ids[at, :], wide[1, at, :]
            for r in range(8):
                hit = jnp.broadcast_to(shell[r : r + 1], (SHELLS, LANES)) == shells
                total = total + jnp.where(
                    hit, jnp.broadcast_to(value[r : r + 1], (SHELLS, LANES)), 0.0
                )
            return total

        by_lane = lax.fori_loop(
            0, lanes_n // 8, add_rows, jnp.zeros((SHELLS, LANES), jnp.float32)
        )
        return lax.dot_general(
            jnp.ones((8, LANES), jnp.float32),
            by_lane,
            (((1,), (1,)), ((), ())),
            precision=lax.Precision.HIGHEST,
            preferred_element_type=jnp.float32,
        )[0:1]

    ahead = 1 if x_n > 1 else 0
    first_head = (me == 0) & (z_hi == 0)

    def forward(xx, zz, c):
        remote(final, final, f_send, f_rsem, me, slab_of(xx, zz, c)).start()

    def forward_all():
        for xx in range(x_n):

            @pl.when(x == xx)
            def _(xx=xx):
                if xx or not ahead:
                    forward(xx, z_hi, 0)
                else:

                    @pl.when(jnp.logical_not(first_head))
                    def _():
                        forward(xx, z_hi, 0)

                if xx == ahead and xx:

                    @pl.when(first_head)
                    def _():
                        forward(0, z_hi, 0)

                @pl.when(late >= heads)
                def _():
                    for to in {0: () if ahead else (0,), 1: (0, 1)}.get(xx, (xx,)):
                        forward(to, late, 1)
                        forward(to, late, 0)

    def forwards_left():
        for xx in range(x_n):
            for is_first in (False, True):
                for has_late in (False, True):
                    copies = 1
                    if xx == 0 and ahead and is_first:
                        copies -= 1
                    if xx == 1 and is_first:
                        copies += 1
                    if has_late:
                        copies += 2 * len({0: () if ahead else (0,), 1: (0, 1)}.get(xx, (xx,)))
                    if copies:

                        @pl.when(
                            (x == xx)
                            & (first_head == is_first)
                            & ((late >= heads) == has_late)
                        )
                        def _(copies=copies):
                            left(many(copies * OUT_ROWS), f_send)

    load_all.wait()

    @pl.when(core == 0)
    def _():
        for some in (far_ones, [*near_ones, 0]):
            for n in range(HALVES):
                for d in some:
                    part_copy(n, d).start()
        load_ids.wait()
        ids_copy().start()
        spec_out[...] = local_spectrum()
        spec_copy().start()

    @pl.when(core == 1)
    def _():
        for some in (far_ones, near_ones):
            for n in range(HALVES):
                for d in some:
                    part_copy(n, d).start()

        first = lax.broadcasted_iota(jnp.int32, (snaps, LANES), 0) < half

        def spread_shells(c):
            for g in range(GROUPS):
                if c == 1:
                    row = all_ids[pl.ds(me * GROUPS + g, 1), :]
                else:
                    row = peer_ids[c // 2, g : g + 1, :]
                row = jnp.broadcast_to(row, (SHELLS, LANES))
                hot = jnp.where(row == shells, 1.0, 0.0).astype(jnp.bfloat16)
                onehot[c, :, g * LANES : (g + 1) * LANES] = hot

        def widen(core_of, n):
            for t in range(snaps):
                for c in range(3):
                    value = recv[core_of, n, t, c].astype(jnp.float32)
                    for at in (t, t + snaps) if t < half else (t,):
                        row = at * PITCH + n * PIECE
                        wide[c, row : row + PIECE, :] = value

        def products(g):
            def rows(c, p, d):
                return wide[c, pl.ds(d * PITCH + 2 * g + p, snaps, stride=PITCH), :]

            def put(k, value):
                terms[k * snaps : (k + 1) * snaps, g * LANES : (g + 1) * LANES] = value.astype(
                    jnp.bfloat16
                )

            own = [[rows(c, p, 0) for p in range(2)] for c in range(3)]
            for d in range(1, half + 1):
                other = [[rows(c, p, d) for p in range(2)] for c in range(3)]
                real = sum(own[c][p] * other[c][p] for c in range(3) for p in range(2))
                imag = sum(own[c][1] * other[c][0] - own[c][0] * other[c][1] for c in range(3))
                if d < half:
                    put(2 * d - 2, real)
                    put(2 * d - 1, imag)
                else:
                    put(2 * d - 2, jnp.where(first, real, imag))

        def bin_part(core_of, q):
            for g in (2 * q, 2 * q + 1):
                products(g)
            modes = slice(2 * q * LANES, 2 * (q + 1) * LANES)
            return lax.dot_general(
                terms[:, modes],
                onehot[core_of, :, modes],
                (((1,), (1,)), ((), ())),
                preferred_element_type=jnp.float32,
            )

        with jax.named_scope("c_onehot"):
            load_ids.wait()
            spread_shells(1)

            @pl.when(z_hi < heads)
            def _():
                arrived(peer_ids.at[0], i_recv.at[0])
                spread_shells(0)

        with jax.named_scope("c_spectrum"):
            mine = local_spectrum()
            spec_copy().wait_recv()
            spec_x[x] = mine + spec_peer[...]
            for d in x_steps:
                remote(
                    spec_x.at[x],
                    spec_x.at[x],
                    t_send,
                    t_rsem,
                    me,
                    slab_of((x + d) % x_n, z_hi, 1),
                ).start()

        quarters = GROUPS // 2 // HALVES

        def work_off(c, n):
            with jax.named_scope(f"d_wait{c}{n}"):
                arrived(recv.at[c, n], m_recv.at[c, n])
            with jax.named_scope(f"e_work{c}{n}"):
                widen(c, n)
                for q in range(n * quarters, (n + 1) * quarters):
                    if (c, q) == (1, 0):
                        binned[...] = bin_part(c, q)
                    else:
                        binned[...] += bin_part(c, q)

        for n in range(HALVES):
            work_off(1, n)

            @pl.when(z_hi < heads)
            def _(n=n):
                work_off(0, n)

        @pl.when((z_hi < heads) & (late >= heads))
        def _():
            arrived(peer_ids.at[1], i_recv.at[1])
            spread_shells(2)
            for n in range(HALVES):
                work_off(2, n)

        with jax.named_scope("g_turn"):
            for k in range(snaps - 1):
                value, shift = binned[k * snaps : (k + 1) * snaps], (k // 2 + 1) // 2
                sums[pl.ds(shift * snaps + k, snaps - shift, stride=snaps), :] = value[
                    0 : snaps - shift
                ]
                if shift:
                    sums[pl.ds(k, shift, stride=snaps), :] = value[snaps - shift :]
            sums[pl.ds(snaps - 1, snaps, stride=snaps), :] = jnp.zeros((snaps, SHELLS), jnp.float32)

        with jax.named_scope("h_owner"):
            for d in y_steps:
                yy = (y + d) % y_n
                remote(
                    sums.at[rows_of(yy, block)],
                    r_recv.at[y],
                    r_send,
                    r_rsem,
                    yy * Z_LO + z_lo,
                    slab,
                ).start()
            r_recv[y] = sums[rows_of(y, block), :]
            if x_n > 1:
                arrived(spec_x.at[pl.ds(0, x_n - 1)], t_rsem)
            spec_recv[me] = ordered_sum([spec_x[i] for i in range(x_n)])
            for d in by_distance:
                remote(
                    spec_recv.at[me], spec_recv.at[me], s_send, s_rsem, there(d), slab
                ).start()
            arrived(r_recv.at[pl.ds(0, y_n - 1)], r_rsem)
            x_recv[x] = ordered_sum([r_recv[i] for i in range(y_n)])

        with jax.named_scope("i_x"):
            for xx in range(x_n):

                @pl.when(x != xx)
                def _(xx=xx):
                    remote(
                        x_recv.at[x], x_recv.at[x], x_send, x_rsem, me, slab_of(xx, z_hi, 1)
                    ).start()

            arrived(spec_recv.at[pl.ds(0, snaps - 1)], s_rsem)
            for t in range(snaps):
                own_src[t : t + 1, :] = spec_recv[t]
            for h in range(heads):

                @pl.when(z_hi != h)
                def _(h=h):
                    remote(
                        own_src, own_recv.at[z_hi], o_send, o_rsem, me, slab_of(x, h, 1)
                    ).start()

                @pl.when(z_hi == h)
                def _(h=h):
                    own_recv[h] = own_src[...]

            if x_n > 1:
                arrived(x_recv.at[pl.ds(0, x_n - 1)], x_rsem)
            total = ordered_sum([x_recv[i] for i in range(x_n)])

        with jax.named_scope("j_pairs"):
            for k in range(Z_LO):
                for d in range(1, half + 1):
                    row = k * snaps + 2 * d - 2
                    pair_src[k, d - 1] = total[row : row + 2]

        def pair_copy(h, k, i, send_sem, recv_sem):
            count = len(pairs_at[i])
            return remote(
                pair_src.at[k, pl.ds(pairs_at[i][0] - 1, count)],
                pair_recv.at[z, slots.index(i), pl.ds(0, count)],
                send_sem,
                recv_sem,
                (base + snaps + k + i) % snaps,
                slab_of(x, h, 1),
            )

        with jax.named_scope("k_send"):
            for h in range(heads):
                for k, i in away:
                    pair_copy(h, k, i, p_send, p_rsem).start()
                for k, i in at_home:
                    here = (z_hi == h) & (z_lo == k + i)

                    @pl.when(here)
                    def _(k=k, i=i):
                        first_pair, count = pairs_at[i][0] - 1, len(pairs_at[i])
                        pair_recv[z, slots.index(i), 0:count] = pair_src[
                            k, first_pair : first_pair + count
                        ]

                    @pl.when(jnp.logical_not(here))
                    def _(h=h, k=k, i=i):
                        pair_copy(h, k, i, h_send, h_rsem).start()

        left(src.at[:, pl.ds(0, (snaps - 1) * ROWS)], m_send)
        left(r_recv.at[pl.ds(0, y_n - 1)], r_send)
        if x_n > 1:
            left(x_recv.at[pl.ds(0, x_n - 1)], x_send)
            left(spec_x.at[pl.ds(0, x_n - 1)], t_send)
        left(spec_recv.at[pl.ds(0, snaps - 1)], s_send)

        @pl.when(z_hi < heads)
        def _():
            with jax.named_scope("l_pairwait"):
                arrived(many(z_n * away_rows // Z_LO), p_rsem)
                arrived(home_rows(z_n - 1), h_rsem)
                if z_hi_n > 1:
                    arrived(own_recv.at[pl.ds(0, z_hi_n - 1)], o_rsem)

            with jax.named_scope("m_coh"):
                load_order.wait()
                own = ordered_sum([own_recv[h] for h in range(z_hi_n)])
                spec_rows[...] = own
                spec = spec_rows[pl.ds(me, 1), :]
                final[snaps : snaps + 1, :] = spec

                def pair(i, d):
                    at = pairs_at[i].index(d)
                    return ordered_sum([pair_recv[p, slots.index(i), at] for p in range(z_n)])

                def power(rows):
                    re, im = rows[0:1], rows[1:2]
                    return re * re + im * im

                def put_row(e, value):
                    power_rows[pl.ds((me + snaps - e) % snaps, 1), :] = value

                put_row(0, spec * spec)
                for d in range(1, half):
                    put_row(d, power(pair((d + 1) // 2, d)))
                    put_row(snaps - d, power(pair(-(d // 2), d)))
                re = pair((half + 1) // 2, half)[0:1]
                im = pair(-(half // 2), half)[0:1]
                put_row(half, re * re + im * im)
                coh_rows[...] = power_rows[...] / (spec * own)
                for j in range(snaps):
                    final[j : j + 1, :] = coh_rows[pl.ds(order_ref[j], 1), :]
                forward_all()

        @pl.when(z_hi >= heads)
        def _():
            with jax.named_scope("n_finalwait"):
                arrived(final, f_rsem)
                load_order.wait()

    @pl.when(core == 0)
    def _():
        with jax.named_scope("n_finalwait"):
            arrived(final, f_rsem)

    with jax.named_scope("o_end"):
        out_ref[...] = final[0 : snaps + 1]
        @pl.when(core == 0)
        def _():
            left(src, m_send)
            left(peer_ids.at[0], i_send)
            left(spec_out, e_send)

        @pl.when(core == 1)
        def _():
            left(many(heads * away_rows), p_send)

            @pl.when(z_hi < heads)
            def _():
                left(home_rows(heads * Z_LO - 1), h_send)
                if heads > 1:
                    left(own_recv.at[pl.ds(0, heads - 1)], o_send)
                forwards_left()

            @pl.when(z_hi >= heads)
            def _():
                left(home_rows(heads * Z_LO), h_send)
                left(own_recv.at[pl.ds(0, heads)], o_send)


def finish(snaps, done_ref, coh_ref, spec_ref, sem):
    coh = pltpu.make_async_copy(done_ref.at[0:snaps], coh_ref.at[0], sem.at[0])
    spec = pltpu.make_async_copy(done_ref.at[snaps : snaps + 1], spec_ref, sem.at[1])
    coh.start()
    spec.start()
    coh.wait()
    spec.wait()


def body(sizes, velocity, shell_index, ref_order):
    snaps, x_n, z_hi_n = sizes
    half = snaps // 2
    heads = min(2, z_hi_n)
    lanes_n = velocity.shape[3] // LANES
    vel = velocity.reshape(3, 2, lanes_n, LANES).transpose(0, 2, 1, 3)
    vel = vel.reshape(3, 2 * lanes_n, LANES)
    ids = shell_index.reshape(lanes_n, LANES)
    f32, bf16, dma = jnp.float32, jnp.bfloat16, pltpu.SemaphoreType.DMA
    done = pl.pallas_call(
        functools.partial(kernel, sizes),
        out_shape=pltpu.VMEM((snaps + 1, SHELLS), f32),
        in_specs=[pl.BlockSpec(memory_space=pl.ANY)] * 3,
        out_specs=pl.BlockSpec(memory_space=pltpu.VMEM),
        scratch_shapes=[
            pltpu.VMEM((3, 2 * lanes_n, LANES), bf16),
            pltpu.VMEM((SETS, HALVES, snaps, 3, PIECE, LANES), bf16),
            pltpu.VMEM((lanes_n, LANES), jnp.int32),
            pltpu.VMEM((2, GROUPS, LANES), jnp.int32),
            pltpu.SMEM((snaps,), jnp.int32),
            pltpu.VMEM((3, (snaps + half + 1) * PITCH, LANES), f32),
            pltpu.VMEM(((snaps - 1) * snaps, GROUPS * LANES), bf16),
            pltpu.VMEM((SETS, SHELLS, GROUPS * LANES), bf16),
            pltpu.VMEM(((snaps - 1) * snaps, SHELLS), f32),
            pltpu.VMEM((snaps * snaps, SHELLS), f32),
            pltpu.VMEM((snaps // Z_LO, Z_LO * snaps, SHELLS), f32),
            pltpu.VMEM((x_n, Z_LO * snaps, SHELLS), f32),
            pltpu.VMEM((1, SHELLS), f32),
            pltpu.VMEM((1, SHELLS), f32),
            pltpu.VMEM((x_n, 1, SHELLS), f32),
            pltpu.VMEM((snaps, 1, SHELLS), f32),
            pltpu.VMEM((snaps, SHELLS), f32),
            pltpu.VMEM((z_hi_n, snaps, SHELLS), f32),
            pltpu.VMEM((Z_LO, half, 2, SHELLS), f32),
            pltpu.VMEM((z_hi_n * Z_LO, half + 1, 2, 2, SHELLS), f32),
            pltpu.VMEM((snaps, SHELLS), f32),
            pltpu.VMEM((snaps, SHELLS), f32),
            pltpu.VMEM((snaps, SHELLS), f32),
            pltpu.VMEM((OUT_ROWS, SHELLS), f32),
            dma((3,)),
            dma(()),
            dma((SETS, HALVES)),
            dma(()),
            dma((2,)),
            *[dma(())] * 18,
        ],
        compiler_params=pltpu.CompilerParams(collective_id=0, has_side_effects=True),
    )(vel, ids, ref_order)
    return pl.pallas_call(
        functools.partial(finish, snaps),
        out_shape=(
            jax.ShapeDtypeStruct((1, snaps, SHELLS), f32),
            jax.ShapeDtypeStruct((1, SHELLS), f32),
        ),
        in_specs=[pl.BlockSpec(memory_space=pltpu.VMEM)],
        out_specs=(pl.BlockSpec(memory_space=pl.ANY),) * 2,
        scratch_shapes=[dma((2,))],
    )(pltpu.with_memory_space_constraint(done, pltpu.VMEM))


def solution(mesh):
    snaps, slabs = mesh.shape["tm"], mesh.shape["slab"]
    z_hi_n = min(Z_HI, slabs // CORES)
    sizes = (snaps, slabs // CORES // z_hi_n, z_hi_n)
    return jax.shard_map(
        functools.partial(body, sizes),
        mesh=mesh,
        in_specs=(P("tm", None, None, "slab"), P("slab"), P()),
        out_specs=(P("tm", None, None), P("tm", None)),
        check_vma=False,
    )
```
